256 devices in a mesh: lat: 32 (over y_hi, z, core), lon: 8 (over y_lo, x).
Axes of the slice: x: 4, y: 4 (y_hi: 2, y_lo: 2; y = y_hi * 2 + y_lo), z: 8, core: 2. Of those that a mesh axis runs over, the one named last changes fastest.
Arguments:
- field: bfloat16 [384, 768, 512], P('lat', 'lon'), may hold values from -6 to 6
- quad_weight: float32 [384], P('lat'), may hold values from 0.5 to 1.5
- legendre: bfloat16 [384, 384, 384], P('lat'), as said below
- filter_real: float32 [384, 512], replicated, may hold values from -4 to 4
- filter_imag: float32 [384, 512], replicated, may hold values from -4 to 4
- neighbour: int32 [384, 12], P('lat'), may hold values from 0 to 24
- basis: int32 [384, 12], P('lat'), may hold values from 0 to 7
- disco_quad: float32 [384, 12], P('lat'), may hold values from 0.5 to 1.5
- disco_weight: float32 [8, 512], replicated, may hold values from -2 to 2
- norm_gain: float32 [512], replicated, may hold values from 0.5 to 1.5
- w_in: bfloat16 [512, 1024], replicated, may hold values from -0.25 to 0.25
- b_in: float32 [1024], replicated, may hold values from -3 to 3
- w_out: bfloat16 [1024, 512], replicated, may hold values from -0.1875 to 0.1875
- b_out: float32 [512], replicated, may hold values from -3 to 3
Outputs:
- block_out: bfloat16 [384, 768, 512], P('lat', 'lon')
- spatial: bfloat16 [384, 768, 512], P('lat', 'lon')
The draws below stay inside these ranges and needn't reach their ends.
Inputs may be any that keep to these rules, and one draw needn't show every extreme that they name: legendre[m, l, t] = 0 for l < m.
All inputs are finite; a program needn't handle non-finite values.
Results may differ from the reference program's by a relative error of at most 0.018.
Values may be sent and summed in bfloat16 or wider, within the bound.
A program may use at most 64 MiB of HBM per device.

```python
import math
import jax
import jax.numpy as jnp
from jax import lax

C = 512
FF = 1024
NLON = 768
HALO = 2
SLOTS = 12
KB = 8
NLAT = 384
MMAX = 384
LMAX = 384
NWIN = 25


def draw_legendre(key, part):
    values = jax.random.normal(key, (MMAX, LMAX, NLAT), jnp.float32)
    values = values * NLAT ** (-0.5)
    waves = jnp.arange(MMAX, dtype=jnp.int32)[:, None, None]
    degrees = jnp.arange(LMAX, dtype=jnp.int32)[None, :, None]
    values = jnp.where(degrees >= waves, values, 0.0)
    return values.astype(jnp.bfloat16)


def set_ends(drawn, key, smallest, largest):
    extent = drawn.shape
    place = [jax.random.randint(jax.random.fold_in(key, axis), (), 0, extent[axis]) for axis in range(len(extent))]
    drawn = drawn.at[tuple(place)].set(smallest)
    longest = extent.index(max(extent))
    place[longest] = (place[longest] + 1) % extent[longest]
    return drawn.at[tuple(place)].set(largest)


def levels(stream_key, extent, cuts, low, top_value):
    loudness = 1.0
    for dim, parts in cuts:
        draws = jax.random.uniform(jax.random.fold_in(jax.random.fold_in(stream_key, 6), dim), (parts,), jnp.float32, low / len(cuts), top_value / len(cuts))
        loudness = loudness * jnp.repeat(jnp.exp(draws), extent[dim] // parts).reshape((-1,) + (1,) * (len(extent) - 1 - dim))
    return loudness


def bell_draw(key, extent, width, limit, cuts=(), kind=jnp.bfloat16):
    gain = levels(key, extent, cuts, -0.22, 0.18) if cuts else 1.0
    entries = jax.random.normal(key, extent, jnp.float32) * width * gain
    return jnp.minimum(jnp.maximum(entries, -limit), limit).astype(kind)


def setup_inputs(seed: int = 0) -> dict:
    splits = jax.random.split(jax.random.key(seed), 15)
    return {
        "field": bell_draw(splits[0], (NLAT, NLON, C), 1.0, 6.0, ((0, 32), (1, 8))),
        "quad_weight": jnp.clip(0.5 + 1.0 * jax.random.uniform(splits[1], (NLAT,), jnp.float32) ** levels(splits[1], (NLAT,), ((0, 32),), -0.2, 0.2), 0.5, 1.5),
        "legendre": draw_legendre(jax.random.fold_in(splits[14], 71), 0),
        "filter_real": bell_draw(splits[3], (LMAX, C), 0.7, 4.0, (), jnp.float32),
        "filter_imag": bell_draw(splits[4], (LMAX, C), 0.7, 4.0, (), jnp.float32),
        "neighbour": set_ends(jax.random.randint(splits[5], (NLAT, SLOTS), 0, NWIN), jax.random.fold_in(splits[5], 1), 0, NWIN - 1).astype(jnp.int32),
        "basis": set_ends(jax.random.randint(splits[6], (NLAT, SLOTS), 0, KB), jax.random.fold_in(splits[6], 1), 0, KB - 1).astype(jnp.int32),
        "disco_quad": jnp.clip(0.5 + 1.0 * jax.random.uniform(splits[7], (NLAT, SLOTS), jnp.float32) ** levels(splits[7], (NLAT, SLOTS), ((0, 32),), -0.2, 0.2), 0.5, 1.5),
        "disco_weight": bell_draw(splits[8], (KB, C), 0.3, 2.0, (), jnp.float32),
        "norm_gain": jnp.clip(1.0 + 0.1 * jax.random.normal(splits[9], (C,), jnp.float32), 0.5, 1.5),
        "w_in": bell_draw(splits[10], (C, FF), C ** -0.5, 0.25),
        "b_in": bell_draw(splits[11], (FF,), 0.5, 3.0, (), jnp.float32),
        "w_out": bell_draw(splits[12], (FF, C), FF ** -0.5, 0.1875),
        "b_out": bell_draw(splits[13], (C,), 0.5, 3.0, (), jnp.float32),
    }


exact_mode = lax.Precision.HIGHEST

def window_kernel(neighbour, basis, disco_quad, disco_weight):
    places = (neighbour[:, :, None] == jnp.arange(NWIN, dtype=jnp.int32)[None, None, :]).astype(jnp.float32)
    places = places * disco_quad[:, :, None]
    kinds = (basis[:, :, None] == jnp.arange(KB, dtype=jnp.int32)[None, None, :]).astype(jnp.float32)
    mixing = jnp.einsum('isn,isb->inb', places, kinds, precision=exact_mode)
    return jnp.einsum('inb,bc->inc', mixing, disco_weight, precision=exact_mode)

def convolve(padded, kernel, lat_rows, lon_cols):
    span = 2 * HALO + 1
    total = jnp.zeros((lat_rows, lon_cols, kernel.shape[2]), jnp.float32)
    for offset in range(NWIN):
        row_shift = offset // span
        col_shift = offset % span
        window = padded[row_shift:row_shift + lat_rows, col_shift:col_shift + lon_cols, :]
        total = total + kernel[:, offset, None, :] * window.astype(jnp.float32)
    return total

def channel_mlp(spatial, field, norm_gain, w_in, b_in, w_out, b_out):
    channels = spatial.shape[-1]
    tokens = spatial.reshape(-1, channels).astype(jnp.float32)
    center = lax.optimization_barrier(jnp.mean(tokens, axis=1, keepdims=True))
    spread = lax.optimization_barrier(jnp.mean((tokens - center) ** 2, axis=1, keepdims=True))
    normed = ((tokens - center) * lax.rsqrt(spread + 1e-05) * norm_gain).astype(jnp.bfloat16)
    hidden = jnp.dot(normed.astype(jnp.float32), w_in.astype(jnp.float32), precision=exact_mode) + b_in
    hidden = jax.nn.gelu(hidden).astype(jnp.bfloat16)
    result = jnp.dot(hidden.astype(jnp.float32), w_out.astype(jnp.float32), precision=exact_mode)
    result = result + b_out + field.reshape(-1, channels).astype(jnp.float32)
    return result.astype(jnp.bfloat16).reshape(field.shape)

def reference(field, quad_weight, legendre, filter_real, filter_imag, neighbour, basis, disco_quad, disco_weight, norm_gain, w_in, b_in, w_out, b_out):
    x_float = field.astype(jnp.float32)
    spectrum = jnp.fft.rfft(x_float, axis=1)[:, :MMAX, :] / math.sqrt(NLON)
    weight = quad_weight[:, None, None]
    weighted = jnp.stack([jnp.real(spectrum) * weight, jnp.imag(spectrum) * weight], axis=1).astype(jnp.bfloat16)
    legend = legendre.astype(jnp.float32)
    coeffs = jnp.einsum('mlt,trmc->lrmc', legend, weighted.astype(jnp.float32), precision=exact_mode)
    gain_real = filter_real[:, None, :]
    gain_imag = filter_imag[:, None, :]
    real_part = coeffs[:, 0]
    imag_part = coeffs[:, 1]
    filtered = jnp.stack([gain_real * real_part - gain_imag * imag_part, gain_real * imag_part + gain_imag * real_part], axis=1).astype(jnp.bfloat16)
    synthesis = jnp.einsum('mlt,lrmc->trmc', legend, filtered.astype(jnp.float32), precision=exact_mode).astype(jnp.bfloat16)
    modes = lax.complex(synthesis[:, 0].astype(jnp.float32), synthesis[:, 1].astype(jnp.float32))
    modes = jnp.pad(modes, ((0, 0), (0, NLON // 2 + 1 - MMAX), (0, 0)))
    wave = (jnp.fft.irfft(modes, n=NLON, axis=1) * math.sqrt(NLON)).astype(jnp.bfloat16)
    kernel = window_kernel(neighbour, basis, disco_quad, disco_weight)
    cycle = jnp.pad(wave, ((0, 0), (HALO, HALO), (0, 0)), mode='wrap')
    padded = jnp.pad(cycle, ((HALO, HALO), (0, 0), (0, 0)))
    conv = convolve(padded, kernel, NLAT, NLON)
    spatial = (wave.astype(jnp.float32) + conv).astype(jnp.bfloat16)
    block_out = channel_mlp(spatial, field, norm_gain, w_in, b_in, w_out, b_out)
    return (block_out, spatial)
```

```python
import functools
import math

import jax
import jax.numpy as jnp
import ml_dtypes
import numpy as np
from jax import lax
from jax.experimental import pallas as pl
from jax.experimental.pallas import tpu as pltpu
from jax.sharding import PartitionSpec as P

HALO = 2
LANES = 128
MESH = pl.DeviceIdType.MESH
BF16 = jnp.bfloat16
F32 = jnp.float32


def tables(nlon, mmax, groups, blocks):
    per = mmax // groups
    waves = np.stack([np.arange(groups) * per + p for p in range(per)])
    waves = np.repeat(waves[:, None, :], 2, axis=1).reshape(-1)
    part = np.broadcast_to(np.array([0, 1])[None, :, None], (per, 2, groups)).reshape(-1)
    cols = nlon // blocks
    edge = np.array([-2, -1, cols, cols + 1])
    halo = (edge[:, None] + np.arange(blocks)[None, :] * cols).reshape(-1) % nlon
    points = np.concatenate([np.arange(nlon), halo])
    angle = (waves[:, None] * points[None, :] % nlon) * (2.0 * math.pi / nlon)
    wave = np.where(part[:, None] == 0, np.cos(angle), -np.sin(angle)) / math.sqrt(nlon)
    factor = np.where(waves == 0, 1.0, 2.0)
    forward = wave[:, :nlon].astype(ml_dtypes.bfloat16)
    inverse = (wave * factor[:, None]).T.astype(ml_dtypes.bfloat16)
    return forward, np.ascontiguousarray(inverse)


class Sizes:
    def __init__(self, mesh, lat_rows, lon_cols, channels, wave_block, degrees):
        self.ni = mesh.shape["lat"]
        self.nj = mesh.shape["lon"]
        self.nq = channels // LANES
        self.nh = self.nj // self.nq
        self.groups = self.ni * self.nh
        self.rows = lat_rows
        self.trow = lat_rows // self.nh
        self.cols = lon_cols
        self.nlon = lon_cols * self.nj
        self.chan = channels
        self.wper = wave_block // self.nh
        self.deg = degrees
        self.nlat = lat_rows * self.ni
        self.step = 2
        self.chunks = self.trow // self.step
        self.mr = 2 * self.wper
        self.blk = self.step * self.mr


def exchange_kernel(
    z,
    quad_ref,
    field_ref,
    leg_ref,
    fr_ref,
    fi_ref,
    fwd_ref,
    inv_ref,
    wave_out,
    edge_out,
    cols_in,
    ltab,
    ltrans,
    fwd,
    inv,
    gr,
    gi,
    stage,
    wide,
    send1,
    recv1,
    send2,
    recv2,
    wbuf,
    ebuf32,
    ebuf,
    load_sem,
    own_sem,
    a_send,
    a_recv,
    b_send,
    b_recv,
    c_send,
    c_recv,
    d_send,
    d_recv,
    e_send,
    e_recv,
    out_own,
    h_send,
    h_recv,
):
    i = lax.axis_index("lat")
    j = lax.axis_index("lon")
    h = j // z.nq
    q = j % z.nq
    me = i * z.nh + h
    lane0 = pl.multiple_of(q * LANES, LANES)
    G = z.groups

    loads = [
        pltpu.make_async_copy(leg_ref.at[pl.ds(h * z.wper, z.wper)], ltab, load_sem.at[0]),
        pltpu.make_async_copy(fwd_ref, fwd, load_sem.at[1]),
        pltpu.make_async_copy(inv_ref, inv, load_sem.at[2]),
        pltpu.make_async_copy(fr_ref.at[:, pl.ds(lane0, LANES)], gr, load_sem.at[3]),
        pltpu.make_async_copy(fi_ref.at[:, pl.ds(lane0, LANES)], gi, load_sem.at[4]),
    ]
    own = pltpu.make_async_copy(
        field_ref.at[pl.ds(h * z.trow, z.trow), :, pl.ds(lane0, LANES)],
        cols_in.at[:, pl.ds(pl.multiple_of(j * z.cols, 16), z.cols), :],
        own_sem,
    )
    loads[1].start()
    own.start()
    for k in (0, 2, 3, 4):
        loads[k].start()

    def group_peer(o):
        nz = max(G // 8, 1)
        a = (o % nz) * 3 % nz
        b = o // nz
        per = G // nz
        here = me // (per // 2) % nz if nz > 1 else 0
        half = me // (G // 2)
        low = me % (per // 2)
        zz = (here + a) % nz
        other = (half * (per // 2) + low + b) % per
        peer = (other // (per // 2)) * (G // 2) + zz * (per // 2) + other % (per // 2)
        return peer

    def group_id(peer):
        return {"lat": peer // z.nh, "lon": (peer % z.nh) * z.nq + q}

    barrier = pltpu.get_barrier_semaphore()

    def greet(o, carry):
        pl.semaphore_signal(
            barrier, inc=1, device_id=group_id(group_peer(o)), device_id_type=MESH
        )
        return carry

    def greet_lon(o, carry):
        hh = (h + o // (z.nq - 1)) % z.nh
        qq = (q + 1 + o % (z.nq - 1)) % z.nq
        pl.semaphore_signal(
            barrier, inc=1, device_id={"lat": i, "lon": hh * z.nq + qq}, device_id_type=MESH
        )
        return carry

    lon_only = z.nh * (z.nq - 1)
    lax.fori_loop(0, lon_only, greet_lon, 0)
    lax.fori_loop(1, G, greet, 0)
    pl.semaphore_wait(barrier, lon_only + G - 1)

    for c in range(z.chunks):

        def send_a(o, carry):
            p = (j + o) % z.nj
            hp = p // z.nq
            qp = p % z.nq
            pltpu.make_async_remote_copy(
                src_ref=field_ref.at[
                    pl.ds(hp * z.trow + c * z.step, z.step),
                    :,
                    pl.ds(pl.multiple_of(qp * LANES, LANES), LANES),
                ],
                dst_ref=cols_in.at[
                    pl.ds(c * z.step, z.step), pl.ds(pl.multiple_of(j * z.cols, 16), z.cols), :
                ],
                send_sem=a_send,
                recv_sem=a_recv.at[c],
                device_id={"lat": i, "lon": p},
                device_id_type=MESH,
            ).start()
            return carry

        lax.fori_loop(1, z.nj, send_a, 0)

    loads[0].wait()
    for w in range(z.wper):
        ltrans[w] = ltab[w].T
    loads[1].wait()
    own.wait()

    def await_bytes(ref, sem):
        pltpu.make_async_copy(ref, ref, sem).wait()

    def pack_and_send(c, send, recv, send_sem, recv_sem, load_block):
        def pack(s, carry):
            send[c, s] = load_block(s).astype(BF16)
            return carry

        lax.fori_loop(0, G, pack, 0, unroll=8)
        recv[c, me] = send[c, me]

        def start(o, carry):
            peer = group_peer(o)
            pltpu.make_async_remote_copy(
                src_ref=send.at[c, peer],
                dst_ref=recv.at[c, me],
                send_sem=send_sem,
                recv_sem=recv_sem.at[c],
                device_id=group_id(peer),
                device_id_type=MESH,
            ).start()
            return carry

        lax.fori_loop(1, G, start, 0)

    for c in range(z.chunks):
        span = z.cols * (z.nj - 1)
        await_bytes(cols_in.at[pl.ds(c * z.step, z.step), pl.ds(0, span), :], a_recv.at[c])
        rhs = jnp.concatenate([cols_in[c * z.step + k] for k in range(z.step)], axis=1)
        spec = jnp.dot(fwd[...], rhs, preferred_element_type=F32)
        for k in range(z.step):
            quad = quad_ref[h * z.trow + c * z.step + k]
            part = spec[:, k * LANES : (k + 1) * LANES] * quad
            for p in range(z.mr):
                stage[pl.ds(k * z.mr + p, G, stride=z.blk), :] = part[p * G : (p + 1) * G]
        pack_and_send(
            c,
            send1,
            recv1,
            b_send,
            b_recv,
            lambda s: stage[pl.ds(pl.multiple_of(s * z.blk, 8), z.blk), :],
        )

    for c in range(z.chunks):
        await_bytes(recv1.at[c, pl.ds(0, G - 1)], b_recv.at[c])

        def unpack(s, carry):
            at = pl.multiple_of(s * (z.blk * z.chunks) + c * z.blk, 8)
            wide[pl.ds(at, z.blk), :] = recv1[c, s].astype(F32)
            return carry

        lax.fori_loop(0, G, unpack, 0, unroll=8)

    for k in (2, 3, 4):
        loads[k].wait()

    for w in range(z.wper):
        weighted = jnp.concatenate(
            [wide[pl.ds(2 * w + r, z.nlat, stride=z.mr), :] for r in range(2)], axis=1
        ).astype(BF16)
        coef = jnp.dot(ltab[w], weighted, preferred_element_type=F32)
        re = coef[:, :LANES]
        im = coef[:, LANES:]
        a = gr[...]
        b = gi[...]
        filt = jnp.concatenate([a * re - b * im, a * im + b * re], axis=1).astype(BF16)
        syn = jnp.dot(ltrans[w], filt, preferred_element_type=F32)
        for r in range(2):
            wide[pl.ds(2 * w + r, z.nlat, stride=z.mr), :] = syn[:, r * LANES : (r + 1) * LANES]

    for c in range(z.chunks):
        pack_and_send(
            c,
            send2,
            recv2,
            c_send,
            c_recv,
            lambda s: wide[
                pl.ds(pl.multiple_of(s * (z.blk * z.chunks) + c * z.blk, 8), z.blk), :
            ],
        )

    own_copies = []
    for c in range(z.chunks):
        await_bytes(recv2.at[c, pl.ds(0, G - 1)], c_recv.at[c])

        def unpack(s, carry):
            stage[pl.ds(pl.multiple_of(s * z.blk, 8), z.blk), :] = recv2[c, s].astype(F32)
            return carry

        lax.fori_loop(0, G, unpack, 0, unroll=8)
        modes = jnp.concatenate(
            [
                jnp.concatenate(
                    [stage[pl.ds(k * z.mr + p, G, stride=z.blk), :] for p in range(z.mr)],
                    axis=0,
                )
                for k in range(z.step)
            ],
            axis=1,
        ).astype(BF16)
        full = jnp.dot(inv[...], modes, preferred_element_type=F32)
        edge_rows = 4 * z.step
        for k in range(z.step):
            half = full[:, k * LANES : (k + 1) * LANES]
            wbuf[c * z.step + k] = half[: z.nlon].astype(BF16)
            for e in range(4):
                at = z.nlon + e * z.nj
                ebuf32[pl.ds(k * 4 + e, z.nj, stride=edge_rows), :] = half[at : at + z.nj]
        for p in range(z.nj):
            ebuf[c, p] = ebuf32[p * edge_rows : (p + 1) * edge_rows, :].astype(BF16).astype(F32)

        row = HALO + h * z.trow + c * z.step

        def wave_pair(p):
            return (
                wbuf.at[
                    pl.ds(c * z.step, z.step), pl.ds(pl.multiple_of(p * z.cols, 16), z.cols), :
                ],
                wave_out.at[pl.ds(row, z.step), :, pl.ds(lane0, LANES)],
            )

        def edge_pair(p):
            return (
                ebuf.at[c, p],
                edge_out.at[
                    pl.ds(pl.multiple_of(row * 4, 8), edge_rows), pl.ds(lane0, LANES)
                ],
            )

        def send_d(o, carry):
            p = (j + o) % z.nj
            for (src, dst), ss, rs in (
                (wave_pair(p), d_send, d_recv.at[c]),
                (edge_pair(p), e_send, e_recv.at[c]),
            ):
                pltpu.make_async_remote_copy(
                    src_ref=src,
                    dst_ref=dst,
                    send_sem=ss,
                    recv_sem=rs,
                    device_id={"lat": i, "lon": p},
                    device_id_type=MESH,
                ).start()
            return carry

        lax.fori_loop(1, z.nj, send_d, 0)
        for n, (src, dst) in enumerate((wave_pair(j), edge_pair(j))):
            copy = pltpu.make_async_copy(src, dst, out_own.at[c, n])
            copy.start()
            own_copies.append(copy)

    for copy in own_copies:
        copy.wait()
    for c in range(z.chunks):
        span = z.cols * (z.nj - 1)
        await_bytes(wbuf.at[pl.ds(c * z.step, z.step), pl.ds(0, span), :], d_recv.at[c])
        await_bytes(ebuf.at[c, pl.ds(0, z.nj - 1)], e_recv.at[c])

    last = z.rows + HALO
    moves = []
    for n, (src_row, dst_row, to) in enumerate(
        ((HALO, last, (i + z.ni - 1) % z.ni), (last - HALO, 0, (i + 1) % z.ni))
    ):
        for f, (src, dst) in enumerate(
            (
                (wave_out.at[pl.ds(src_row, HALO)], wave_out.at[pl.ds(dst_row, HALO)]),
                (
                    edge_out.at[pl.ds(src_row * 4, HALO * 4)],
                    edge_out.at[pl.ds(dst_row * 4, HALO * 4)],
                ),
            )
        ):
            move = pltpu.make_async_remote_copy(
                src_ref=src,
                dst_ref=dst,
                send_sem=h_send.at[n, f],
                recv_sem=h_recv.at[n, f],
                device_id={"lat": to, "lon": j},
                device_id_type=MESH,
            )
            move.start()
            moves.append(move)
    for move in moves:
        move.wait()

    span = z.cols * (z.nj - 1)
    await_bytes(wbuf.at[:, pl.ds(0, span), :], a_send)
    await_bytes(send1.at[:, pl.ds(0, G - 1)], b_send)
    await_bytes(send2.at[:, pl.ds(0, G - 1)], c_send)
    await_bytes(wbuf.at[:, pl.ds(0, span), :], d_send)
    await_bytes(ebuf.at[:, pl.ds(0, z.nj - 1)], e_send)


def exchange(z, field, quad, legendre, fr, fi, fwd, inv):
    hbm = pl.BlockSpec(memory_space=pl.ANY)
    dma = pltpu.SemaphoreType.DMA
    flat = z.groups * z.blk
    span = z.rows + 2 * HALO
    return pl.pallas_call(
        functools.partial(exchange_kernel, z),
        name="exchange",
        out_shape=(
            jax.ShapeDtypeStruct((span, z.cols, z.chan), BF16),
            jax.ShapeDtypeStruct((span * 4, z.chan), F32),
        ),
        in_specs=[pl.BlockSpec(memory_space=pltpu.SMEM)] + [hbm] * 6,
        out_specs=(hbm, hbm),
        scratch_shapes=[
            pltpu.VMEM((z.trow, z.nlon, LANES), BF16),
            pltpu.VMEM((z.wper, z.deg, z.nlat), BF16),
            pltpu.VMEM((z.wper, z.nlat, z.deg), BF16),
            pltpu.VMEM(fwd.shape, BF16),
            pltpu.VMEM(inv.shape, BF16),
            pltpu.VMEM((z.deg, LANES), F32),
            pltpu.VMEM((z.deg, LANES), F32),
            pltpu.VMEM((flat, LANES), F32),
            pltpu.VMEM((flat * z.chunks, LANES), F32),
            pltpu.VMEM((z.chunks, z.groups, z.blk, LANES), BF16),
            pltpu.VMEM((z.chunks, z.groups, z.blk, LANES), BF16),
            pltpu.VMEM((z.chunks, z.groups, z.blk, LANES), BF16),
            pltpu.VMEM((z.chunks, z.groups, z.blk, LANES), BF16),
            pltpu.VMEM((z.trow, z.nlon, LANES), BF16),
            pltpu.VMEM((z.nj * 4 * z.step, LANES), F32),
            pltpu.VMEM((z.chunks, z.nj, 4 * z.step, LANES), F32),
            dma((5,)),
            dma,
            dma,
            dma((z.chunks,)),
            dma,
            dma((z.chunks,)),
            dma,
            dma((z.chunks,)),
            dma,
            dma((z.chunks,)),
            dma,
            dma((z.chunks,)),
            dma((z.chunks, 2)),
            dma((2, 2)),
            dma((2, 2)),
        ],
        compiler_params=pltpu.CompilerParams(
            collective_id=0, has_side_effects=True, vmem_limit_bytes=60 << 20
        ),
        cost_estimate=pl.CostEstimate(
            flops=4 * z.trow * z.nlon * z.nlon * LANES, bytes_accessed=1 << 24, transcendentals=0
        ),
    )(quad, field, legendre, fr, fi, fwd, inv)


def local_kernel(
    z,
    rstep,
    neighbour,
    basis,
    quad,
    place,
    wave_ref,
    edge_ref,
    field_ref,
    weight_ref,
    gain_ref,
    win_ref,
    bin_ref,
    wout_ref,
    bout_ref,
    out_ref,
    spatial_ref,
    padded,
):
    g = pl.program_id(0)
    span = z.rows + 2 * HALO
    slots = neighbour.shape[1]

    @pl.when(g == 0)
    def _():
        def widen(pair, carry):
            for q in range(z.nq):
                lanes = slice(q * LANES, (q + 1) * LANES)
                edges = edge_ref[pl.ds(pl.multiple_of(pair * 8, 8), 8), lanes]
                for k in range(2):
                    t = pair * 2 + k
                    padded[t, q, 8 : 8 + z.cols, :] = wave_ref[t, :, lanes].astype(F32)
                    padded[t, q, 6:8, :] = edges[4 * k : 4 * k + 2]
                    padded[t, q, 8 + z.cols : 10 + z.cols, :] = edges[4 * k + 2 : 4 * k + 4]
            return carry

        lax.fori_loop(0, span // 2, widen, 0)

        @pl.when(place[0] == 0)
        def _():
            padded[:HALO] = jnp.zeros((HALO,) + padded.shape[1:], F32)

        @pl.when(place[0] == z.ni - 1)
        def _():
            padded[span - HALO :] = jnp.zeros((HALO,) + padded.shape[1:], F32)

    def conv_row(k, carry):
        t = g * rstep + k
        for q in range(z.nq):
            lanes = slice(q * LANES, (q + 1) * LANES)
            total = padded[t + HALO, q, 8 : 8 + z.cols, :]
            for s in range(slots):
                n = neighbour[t, s]
                coef = weight_ref[basis[t, s], :, lanes] * quad[t, s]
                total = total + coef * padded[t + n // 5, q, pl.ds(6 + n % 5, z.cols), :]
            spatial_ref[k, :, lanes] = total.astype(BF16)
        return carry

    lax.fori_loop(0, rstep, conv_row, 0)
    tokens = spatial_ref[...].reshape(rstep * z.cols, z.chan).astype(F32)
    center = jnp.mean(tokens, axis=1, keepdims=True)
    tokens = tokens - center
    spread = jnp.mean(tokens * tokens, axis=1, keepdims=True)
    normed = (tokens * lax.rsqrt(spread + 1e-05) * gain_ref[...]).astype(BF16)
    hidden = jnp.dot(normed, win_ref[...], preferred_element_type=F32) + bin_ref[...]
    hidden = jax.nn.gelu(hidden).astype(BF16)
    result = jnp.dot(hidden, wout_ref[...], preferred_element_type=F32)
    result = result + bout_ref[...] + field_ref[...].reshape(tokens.shape).astype(F32)
    out_ref[...] = result.astype(BF16).reshape(out_ref.shape)


def local(z, wave, edge, field, neighbour, basis, quad, weight, gain, w_in, b_in, w_out, b_out):
    rstep = 2
    smem = pl.BlockSpec(memory_space=pltpu.SMEM)
    rows = pl.BlockSpec((rstep, z.cols, z.chan), lambda g: (g, 0, 0))

    def whole(x):
        return pl.BlockSpec(x.shape, lambda g: (0,) * x.ndim)

    span = z.rows + 2 * HALO
    place = lax.axis_index("lat").astype(jnp.int32)[None]
    gain, b_in, b_out, weight = gain[None], b_in[None], b_out[None], weight[:, None, :]
    shape = jax.ShapeDtypeStruct(field.shape, BF16)
    return pl.pallas_call(
        functools.partial(local_kernel, z, rstep),
        name="local",
        grid=(z.rows // rstep,),
        out_shape=(shape, shape),
        in_specs=[smem] * 4
        + [whole(wave), whole(edge), rows]
        + [whole(x) for x in (weight, gain, w_in, b_in, w_out, b_out)],
        out_specs=(rows, rows),
        scratch_shapes=[pltpu.VMEM((span, z.nq, z.cols + 16, LANES), F32)],
        compiler_params=pltpu.CompilerParams(vmem_limit_bytes=48 << 20),
    )(
        neighbour,
        basis,
        quad,
        place,
        wave,
        edge,
        field,
        weight,
        gain,
        w_in,
        b_in,
        w_out,
        b_out,
    )


def shards(
    mesh,
    field,
    quad_weight,
    legendre,
    filter_real,
    filter_imag,
    neighbour,
    basis,
    disco_quad,
    disco_weight,
    norm_gain,
    w_in,
    b_in,
    w_out,
    b_out,
):
    lat_rows, lon_cols, channels = field.shape
    z = Sizes(mesh, lat_rows, lon_cols, channels, legendre.shape[0], legendre.shape[1])
    fwd, inv = tables(z.nlon, z.wper * z.groups, z.groups, z.nj)
    wave, edge = exchange(
        z, field, quad_weight, legendre, filter_real, filter_imag, jnp.asarray(fwd), jnp.asarray(inv)
    )
    return local(
        z,
        wave,
        edge,
        field,
        neighbour,
        basis,
        disco_quad,
        disco_weight,
        norm_gain,
        w_in,
        b_in,
        w_out,
        b_out,
    )


def solution(mesh):
    placed = (
        P("lat", "lon", None),
        P("lat"),
        P("lat", None, None),
        P(),
        P(),
        P("lat", None),
        P("lat", None),
        P("lat", None),
        P(),
        P(),
        P(),
        P(),
        P(),
        P(),
    )
    return jax.shard_map(
        functools.partial(shards, mesh),
        mesh=mesh,
        in_specs=placed,
        out_specs=(P("lat", "lon", None), P("lat", "lon", None)),
        check_vma=False,
    )
```

```python
import functools
import math

import jax
import jax.numpy as jnp
import ml_dtypes
import numpy as np
from jax import lax
from jax.experimental import pallas as pl
from jax.experimental.pallas import tpu as pltpu
from jax.sharding import PartitionSpec as P

HALO = 2
LANES = 128
MESH = pl.DeviceIdType.MESH
BF16 = jnp.bfloat16
F32 = jnp.float32


def tables(nlon, mmax, groups, blocks):
    per = mmax // groups
    waves = np.stack([np.arange(groups) * per + p for p in range(per)])
    waves = np.repeat(waves[:, None, :], 2, axis=1).reshape(-1)
    part = np.broadcast_to(np.array([0, 1])[None, :, None], (per, 2, groups)).reshape(-1)
    cols = nlon // blocks
    edge = np.array([-2, -1, cols, cols + 1])
    halo = (edge[:, None] + np.arange(blocks)[None, :] * cols).reshape(-1) % nlon
    points = np.concatenate([np.arange(nlon), halo])
    angle = (waves[:, None] * points[None, :] % nlon) * (2.0 * math.pi / nlon)
    wave = np.where(part[:, None] == 0, np.cos(angle), -np.sin(angle)) / math.sqrt(nlon)
    factor = np.where(waves == 0, 1.0, 2.0)
    forward = wave[:, :nlon].astype(ml_dtypes.bfloat16)
    inverse = (wave * factor[:, None]).T.astype(ml_dtypes.bfloat16)
    return forward, np.ascontiguousarray(inverse)


class Sizes:
    def __init__(self, mesh, lat_rows, lon_cols, channels, wave_block, degrees):
        self.ni = mesh.shape["lat"]
        self.nj = mesh.shape["lon"]
        self.nq = channels // LANES
        self.nh = self.nj // self.nq
        self.groups = self.ni * self.nh
        self.rows = lat_rows
        self.trow = lat_rows // self.nh
        self.cols = lon_cols
        self.nlon = lon_cols * self.nj
        self.chan = channels
        self.wper = wave_block // self.nh
        self.deg = degrees
        self.nlat = lat_rows * self.ni
        self.step = 2
        self.chunks = self.trow // self.step
        self.mr = 2 * self.wper
        self.blk = self.step * self.mr
        self.deep = max(self.groups // 8, 1)

    def turn(self, c, half):
        return c + half * (self.chunks - 1 - 2 * c)


def exchange_kernel(
    z,
    quad_ref,
    field_ref,
    leg_ref,
    fr_ref,
    fi_ref,
    fwd_ref,
    inv_ref,
    wave_out,
    edge_out,
    cols_in,
    ltab,
    ltrans,
    fwd,
    inv,
    gr,
    gi,
    stage,
    wide,
    send1,
    recv1,
    send2,
    recv2,
    wbuf,
    ebuf32,
    ebuf,
    load_sem,
    own_sem,
    a_send,
    a_recv,
    b_send,
    b_recv,
    c_send,
    c_recv,
    d_send,
    d_recv,
    e_send,
    e_recv,
    out_own,
    h_send,
    h_recv,
):
    i = lax.axis_index("lat")
    j = lax.axis_index("lon")
    h = j // z.nq
    q = j % z.nq
    me = i * z.nh + h
    lane0 = pl.multiple_of(q * LANES, LANES)
    G = z.groups

    loads = [
        pltpu.make_async_copy(leg_ref.at[pl.ds(h * z.wper, z.wper)], ltab, load_sem.at[0]),
        pltpu.make_async_copy(fwd_ref, fwd, load_sem.at[1]),
        pltpu.make_async_copy(inv_ref, inv, load_sem.at[2]),
        pltpu.make_async_copy(fr_ref.at[:, pl.ds(lane0, LANES)], gr, load_sem.at[3]),
        pltpu.make_async_copy(fi_ref.at[:, pl.ds(lane0, LANES)], gi, load_sem.at[4]),
    ]
    own = pltpu.make_async_copy(
        field_ref.at[pl.ds(h * z.trow, z.trow), :, pl.ds(lane0, LANES)],
        cols_in.at[:, pl.ds(pl.multiple_of(j * z.cols, 16), z.cols), :],
        own_sem,
    )
    loads[1].start()
    own.start()
    for k in (0, 2, 3, 4):
        loads[k].start()

    low = G // z.deep // 2
    deep = lax.rem(lax.div(me, low), z.deep)
    flat = lax.div(me, G // 2) * low + lax.rem(me, low)
    levels = [lax.rem(deep + 3 * a % z.deep, z.deep) for a in range(z.deep)]

    def each_peer(act):
        def shift(b, skip):
            other = lax.rem(flat + b, 2 * low)
            half = lax.div(other, low)
            side = lax.rem(other, low)
            column = lax.rem(side, z.nh) * z.nq + q
            first = half * (G // 2) + side
            row = half * (z.ni // 2) + lax.div(side, z.nh)
            for a in range(skip, z.deep):
                act(
                    first + levels[a] * low,
                    {"lat": row + levels[a] * (low // z.nh), "lon": column},
                )

        def body(b, carry):
            shift(b, 0)
            return carry

        shift(0, 1)
        lax.fori_loop(1, 2 * low, body, 0)

    barrier = pltpu.get_barrier_semaphore()

    def greet_lon(o, carry):
        hh = (h + o // (z.nq - 1)) % z.nh
        qq = (q + 1 + o % (z.nq - 1)) % z.nq
        pl.semaphore_signal(
            barrier, inc=1, device_id={"lat": i, "lon": hh * z.nq + qq}, device_id_type=MESH
        )
        return carry

    lon_only = z.nh * (z.nq - 1)
    lax.fori_loop(0, lon_only, greet_lon, 0)
    each_peer(
        lambda peer, to: pl.semaphore_signal(
            barrier, inc=1, device_id=to, device_id_type=MESH
        )
    )
    with jax.named_scope("barrier"):
        pl.semaphore_wait(barrier, lon_only + G - 1)

    for c in range(z.chunks):

        def send_a(o, carry):
            p = (j + o) % z.nj
            hp = p // z.nq
            qp = p % z.nq
            pltpu.make_async_remote_copy(
                src_ref=field_ref.at[
                    pl.ds(hp * z.trow + c * z.step, z.step),
                    :,
                    pl.ds(pl.multiple_of(qp * LANES, LANES), LANES),
                ],
                dst_ref=cols_in.at[
                    pl.ds(c * z.step, z.step), pl.ds(pl.multiple_of(j * z.cols, 16), z.cols), :
                ],
                send_sem=a_send,
                recv_sem=a_recv.at[c],
                device_id={"lat": i, "lon": p},
                device_id_type=MESH,
            ).start()
            return carry

        with jax.named_scope("a_start"):
            lax.fori_loop(1, z.nj, send_a, 0)

    loads[0].wait()
    with jax.named_scope("trans"):
        for w in range(z.wper):
            ltrans[w] = ltab[w].T
    loads[1].wait()
    own.wait()

    def await_bytes(ref, sem):
        pltpu.make_async_copy(ref, ref, sem).wait()

    def pack_and_send(c, send, recv, send_sem, recv_sem, load_block):
        def pack(s, carry):
            send[c, s] = load_block(s).astype(BF16)
            return carry

        with jax.named_scope("pack"):
            lax.fori_loop(0, G, pack, 0, unroll=8)
        recv[c, me] = send[c, me]

        def start(peer, to):
            pltpu.make_async_remote_copy(
                src_ref=send.at[c, peer],
                dst_ref=recv.at[c, me],
                send_sem=send_sem,
                recv_sem=recv_sem.at[c],
                device_id=to,
                device_id_type=MESH,
            ).start()

        with jax.named_scope("bc_start"):
            each_peer(start)

    for c in range(z.chunks):
        span = z.cols * (z.nj - 1)
        with jax.named_scope("a_wait"):
            await_bytes(cols_in.at[pl.ds(c * z.step, z.step), pl.ds(0, span), :], a_recv.at[c])
        with jax.named_scope("dft"):
            rhs = jnp.concatenate([cols_in[c * z.step + k] for k in range(z.step)], axis=1)
            spec = jnp.dot(fwd[...], rhs, preferred_element_type=F32)
            for k in range(z.step):
                quad = quad_ref[h * z.trow + c * z.step + k]
                part = spec[:, k * LANES : (k + 1) * LANES] * quad
                for p in range(z.mr):
                    stage[pl.ds(k * z.mr + p, G, stride=z.blk), :] = part[p * G : (p + 1) * G]
        pack_and_send(
            c,
            send1,
            recv1,
            b_send,
            b_recv,
            lambda s: stage[pl.ds(pl.multiple_of(s * z.blk, 8), z.blk), :],
        )

    for c in range(z.chunks):
        with jax.named_scope("b_wait"):
            await_bytes(recv1.at[c, pl.ds(0, G - 1)], b_recv.at[c])

        def unpack(s, carry):
            at = pl.multiple_of(s * (z.blk * z.chunks) + c * z.blk, 8)
            wide[pl.ds(at, z.blk), :] = recv1[c, s].astype(F32)
            return carry

        lax.fori_loop(0, G, unpack, 0, unroll=8)

    for k in (2, 3, 4):
        loads[k].wait()

    with jax.named_scope("legendre"):
        for w in range(z.wper):
            weighted = jnp.concatenate(
                [wide[pl.ds(2 * w + r, z.nlat, stride=z.mr), :] for r in range(2)], axis=1
            ).astype(BF16)
            coef = jnp.dot(ltab[w], weighted, preferred_element_type=F32)
            re = coef[:, :LANES]
            im = coef[:, LANES:]
            a = gr[...]
            b = gi[...]
            filt = jnp.concatenate([a * re - b * im, a * im + b * re], axis=1).astype(BF16)
            syn = jnp.dot(ltrans[w], filt, preferred_element_type=F32)
            for r in range(2):
                wide[pl.ds(2 * w + r, z.nlat, stride=z.mr), :] = syn[:, r * LANES : (r + 1) * LANES]

    for c in range(z.chunks):
        pack_and_send(
            c,
            send2,
            recv2,
            c_send,
            c_recv,
            lambda s: wide[
                pl.ds(
                    pl.multiple_of(
                        s * (z.blk * z.chunks) + z.turn(c, lax.rem(s, z.nh)) * z.blk, 8
                    ),
                    z.blk,
                ),
                :,
            ],
        )

    own_copies = []
    moves = []

    def await_rows(c):
        span = z.cols * (z.nj - 1)
        own_copies[2 * c].wait()
        own_copies[2 * c + 1].wait()
        await_bytes(wbuf.at[pl.ds(c * z.step, z.step), pl.ds(0, span), :], d_recv.at[c])
        await_bytes(ebuf.at[c, pl.ds(0, z.nj - 1)], e_recv.at[c])

    for c in range(z.chunks):
        with jax.named_scope("c_wait"):
            await_bytes(recv2.at[c, pl.ds(0, G - 1)], c_recv.at[c])

        def unpack(s, carry):
            stage[pl.ds(pl.multiple_of(s * z.blk, 8), z.blk), :] = recv2[c, s].astype(F32)
            return carry

        with jax.named_scope("idft"):
            lax.fori_loop(0, G, unpack, 0, unroll=8)
            modes = jnp.concatenate(
                [
                    jnp.concatenate(
                        [stage[pl.ds(k * z.mr + p, G, stride=z.blk), :] for p in range(z.mr)],
                        axis=0,
                    )
                    for k in range(z.step)
                ],
                axis=1,
            ).astype(BF16)
            full = jnp.dot(inv[...], modes, preferred_element_type=F32)
            edge_rows = 4 * z.step
            for k in range(z.step):
                half = full[:, k * LANES : (k + 1) * LANES]
                wbuf[c * z.step + k] = half[: z.nlon].astype(BF16)
                for e in range(4):
                    at = z.nlon + e * z.nj
                    ebuf32[pl.ds(k * 4 + e, z.nj, stride=edge_rows), :] = half[at : at + z.nj]
            for p in range(z.nj):
                ebuf[c, p] = ebuf32[p * edge_rows : (p + 1) * edge_rows, :].astype(BF16).astype(F32)

        row = HALO + h * z.trow + z.turn(c, h) * z.step

        def wave_pair(p):
            return (
                wbuf.at[
                    pl.ds(c * z.step, z.step), pl.ds(pl.multiple_of(p * z.cols, 16), z.cols), :
                ],
                wave_out.at[pl.ds(row, z.step), :, pl.ds(lane0, LANES)],
            )

        def edge_pair(p):
            return (
                ebuf.at[c, p],
                edge_out.at[
                    pl.ds(pl.multiple_of(row * 4, 8), edge_rows), pl.ds(lane0, LANES)
                ],
            )

        def send_d(o, carry):
            p = (j + o) % z.nj
            for (src, dst), ss, rs in (
                (wave_pair(p), d_send, d_recv.at[c]),
                (edge_pair(p), e_send, e_recv.at[c]),
            ):
                pltpu.make_async_remote_copy(
                    src_ref=src,
                    dst_ref=dst,
                    send_sem=ss,
                    recv_sem=rs,
                    device_id={"lat": i, "lon": p},
                    device_id_type=MESH,
                ).start()
            return carry

        with jax.named_scope("d_start"):
            lax.fori_loop(1, z.nj, send_d, 0)
        for n, (src, dst) in enumerate((wave_pair(j), edge_pair(j))):
            copy = pltpu.make_async_copy(src, dst, out_own.at[c, n])
            copy.start()
            own_copies.append(copy)

        if c != 1:
            continue
        with jax.named_scope("h_start"):
            await_rows(0)
        last = z.rows + HALO
        for n, (src_row, dst_row, to) in enumerate(
            ((HALO, last, (i + z.ni - 1) % z.ni), (last - HALO, 0, (i + 1) % z.ni))
        ):
            for f, (src, dst) in enumerate(
                (
                    (wave_out.at[pl.ds(src_row, HALO)], wave_out.at[pl.ds(dst_row, HALO)]),
                    (
                        edge_out.at[pl.ds(src_row * 4, HALO * 4)],
                        edge_out.at[pl.ds(dst_row * 4, HALO * 4)],
                    ),
                )
            ):
                move = pltpu.make_async_remote_copy(
                    src_ref=src,
                    dst_ref=dst,
                    send_sem=h_send.at[n, f],
                    recv_sem=h_recv.at[n, f],
                    device_id={"lat": to, "lon": j},
                    device_id_type=MESH,
                )
                move.start()
                moves.append(move)

    with jax.named_scope("d_wait"):
        for c in range(1, z.chunks):
            await_rows(c)
    with jax.named_scope("h_wait"):
        for move in moves:
            move.wait()

    span = z.cols * (z.nj - 1)
    with jax.named_scope("drain"):
        await_bytes(wbuf.at[:, pl.ds(0, span), :], a_send)
        await_bytes(send1.at[:, pl.ds(0, G - 1)], b_send)
        await_bytes(send2.at[:, pl.ds(0, G - 1)], c_send)
        await_bytes(wbuf.at[:, pl.ds(0, span), :], d_send)
        await_bytes(ebuf.at[:, pl.ds(0, z.nj - 1)], e_send)


def exchange(z, field, quad, legendre, fr, fi, fwd, inv):
    hbm = pl.BlockSpec(memory_space=pl.ANY)
    dma = pltpu.SemaphoreType.DMA
    flat = z.groups * z.blk
    span = z.rows + 2 * HALO
    return pl.pallas_call(
        functools.partial(exchange_kernel, z),
        name="exchange",
        out_shape=(
            jax.ShapeDtypeStruct((span, z.cols, z.chan), BF16),
            jax.ShapeDtypeStruct((span * 4, z.chan), F32),
        ),
        in_specs=[pl.BlockSpec(memory_space=pltpu.SMEM)] + [hbm] * 6,
        out_specs=(hbm, hbm),
        scratch_shapes=[
            pltpu.VMEM((z.trow, z.nlon, LANES), BF16),
            pltpu.VMEM((z.wper, z.deg, z.nlat), BF16),
            pltpu.VMEM((z.wper, z.nlat, z.deg), BF16),
            pltpu.VMEM(fwd.shape, BF16),
            pltpu.VMEM(inv.shape, BF16),
            pltpu.VMEM((z.deg, LANES), F32),
            pltpu.VMEM((z.deg, LANES), F32),
            pltpu.VMEM((flat, LANES), F32),
            pltpu.VMEM((flat * z.chunks, LANES), F32),
            pltpu.VMEM((z.chunks, z.groups, z.blk, LANES), BF16),
            pltpu.VMEM((z.chunks, z.groups, z.blk, LANES), BF16),
            pltpu.VMEM((z.chunks, z.groups, z.blk, LANES), BF16),
            pltpu.VMEM((z.chunks, z.groups, z.blk, LANES), BF16),
            pltpu.VMEM((z.trow, z.nlon, LANES), BF16),
            pltpu.VMEM((z.nj * 4 * z.step, LANES), F32),
            pltpu.VMEM((z.chunks, z.nj, 4 * z.step, LANES), F32),
            dma((5,)),
            dma,
            dma,
            dma((z.chunks,)),
            dma,
            dma((z.chunks,)),
            dma,
            dma((z.chunks,)),
            dma,
            dma((z.chunks,)),
            dma,
            dma((z.chunks,)),
            dma((z.chunks, 2)),
            dma((2, 2)),
            dma((2, 2)),
        ],
        compiler_params=pltpu.CompilerParams(
            collective_id=0, has_side_effects=True, vmem_limit_bytes=60 << 20
        ),
        cost_estimate=pl.CostEstimate(
            flops=4 * z.trow * z.nlon * z.nlon * LANES, bytes_accessed=1 << 24, transcendentals=0
        ),
    )(quad, field, legendre, fr, fi, fwd, inv)


def local_kernel(
    z,
    rstep,
    neighbour,
    basis,
    quad,
    place,
    wave_ref,
    edge_ref,
    field_ref,
    weight_ref,
    gain_ref,
    win_ref,
    bin_ref,
    wout_ref,
    bout_ref,
    out_ref,
    spatial_ref,
    padded,
):
    g = pl.program_id(0)
    span = z.rows + 2 * HALO
    slots = neighbour.shape[1]

    @pl.when(g == 0)
    def _():
        def widen(pair, carry):
            for q in range(z.nq):
                lanes = slice(q * LANES, (q + 1) * LANES)
                edges = edge_ref[pl.ds(pl.multiple_of(pair * 8, 8), 8), lanes]
                for k in range(2):
                    t = pair * 2 + k
                    padded[t, q, 8 : 8 + z.cols, :] = wave_ref[t, :, lanes].astype(F32)
                    padded[t, q, 6:8, :] = edges[4 * k : 4 * k + 2]
                    padded[t, q, 8 + z.cols : 10 + z.cols, :] = edges[4 * k + 2 : 4 * k + 4]
            return carry

        lax.fori_loop(0, span // 2, widen, 0)

        @pl.when(place[0] == 0)
        def _():
            padded[:HALO] = jnp.zeros((HALO,) + padded.shape[1:], F32)

        @pl.when(place[0] == z.ni - 1)
        def _():
            padded[span - HALO :] = jnp.zeros((HALO,) + padded.shape[1:], F32)

    def conv_row(k, carry):
        t = g * rstep + k
        for q in range(z.nq):
            lanes = slice(q * LANES, (q + 1) * LANES)
            total = padded[t + HALO, q, 8 : 8 + z.cols, :]
            for s in range(slots):
                n = neighbour[t, s]
                coef = weight_ref[basis[t, s], :, lanes] * quad[t, s]
                total = total + coef * padded[t + n // 5, q, pl.ds(6 + n % 5, z.cols), :]
            spatial_ref[k, :, lanes] = total.astype(BF16)
        return carry

    lax.fori_loop(0, rstep, conv_row, 0)
    tokens = spatial_ref[...].reshape(rstep * z.cols, z.chan).astype(F32)
    center = jnp.mean(tokens, axis=1, keepdims=True)
    tokens = tokens - center
    spread = jnp.mean(tokens * tokens, axis=1, keepdims=True)
    normed = (tokens * lax.rsqrt(spread + 1e-05) * gain_ref[...]).astype(BF16)
    hidden = jnp.dot(normed, win_ref[...], preferred_element_type=F32) + bin_ref[...]
    hidden = jax.nn.gelu(hidden).astype(BF16)
    result = jnp.dot(hidden, wout_ref[...], preferred_element_type=F32)
    result = result + bout_ref[...] + field_ref[...].reshape(tokens.shape).astype(F32)
    out_ref[...] = result.astype(BF16).reshape(out_ref.shape)


def local(z, wave, edge, field, neighbour, basis, quad, weight, gain, w_in, b_in, w_out, b_out):
    rstep = 2
    smem = pl.BlockSpec(memory_space=pltpu.SMEM)
    rows = pl.BlockSpec((rstep, z.cols, z.chan), lambda g: (g, 0, 0))

    def whole(x):
        return pl.BlockSpec(x.shape, lambda g: (0,) * x.ndim)

    span = z.rows + 2 * HALO
    place = lax.axis_index("lat").astype(jnp.int32)[None]
    gain, b_in, b_out, weight = gain[None], b_in[None], b_out[None], weight[:, None, :]
    shape = jax.ShapeDtypeStruct(field.shape, BF16)
    return pl.pallas_call(
        functools.partial(local_kernel, z, rstep),
        name="local",
        grid=(z.rows // rstep,),
        out_shape=(shape, shape),
        in_specs=[smem] * 4
        + [whole(wave), whole(edge), rows]
        + [whole(x) for x in (weight, gain, w_in, b_in, w_out, b_out)],
        out_specs=(rows, rows),
        scratch_shapes=[pltpu.VMEM((span, z.nq, z.cols + 16, LANES), F32)],
        compiler_params=pltpu.CompilerParams(vmem_limit_bytes=48 << 20),
    )(
        neighbour,
        basis,
        quad,
        place,
        wave,
        edge,
        field,
        weight,
        gain,
        w_in,
        b_in,
        w_out,
        b_out,
    )


def shards(
    mesh,
    field,
    quad_weight,
    legendre,
    filter_real,
    filter_imag,
    neighbour,
    basis,
    disco_quad,
    disco_weight,
    norm_gain,
    w_in,
    b_in,
    w_out,
    b_out,
):
    lat_rows, lon_cols, channels = field.shape
    z = Sizes(mesh, lat_rows, lon_cols, channels, legendre.shape[0], legendre.shape[1])
    fwd, inv = tables(z.nlon, z.wper * z.groups, z.groups, z.nj)
    wave, edge = exchange(
        z, field, quad_weight, legendre, filter_real, filter_imag, jnp.asarray(fwd), jnp.asarray(inv)
    )
    return local(
        z,
        wave,
        edge,
        field,
        neighbour,
        basis,
        disco_quad,
        disco_weight,
        norm_gain,
        w_in,
        b_in,
        w_out,
        b_out,
    )


def solution(mesh):
    placed = (
        P("lat", "lon", None),
        P("lat"),
        P("lat", None, None),
        P(),
        P(),
        P("lat", None),
        P("lat", None),
        P("lat", None),
        P(),
        P(),
        P(),
        P(),
        P(),
        P(),
    )
    return jax.shard_map(
        functools.partial(shards, mesh),
        mesh=mesh,
        in_specs=placed,
        out_specs=(P("lat", "lon", None), P("lat", "lon", None)),
        check_vma=False,
    )
```

```python
import functools
import math

import jax
import jax.numpy as jnp
import ml_dtypes
import numpy as np
from jax import lax
from jax.experimental import pallas as pl
from jax.experimental.pallas import tpu as pltpu
from jax.sharding import PartitionSpec as P

HALO = 2
LANES = 128
MESH = pl.DeviceIdType.MESH
BF16 = jnp.bfloat16
F32 = jnp.float32


def tables(nlon, mmax, groups, blocks):
    per = mmax // groups
    waves = np.stack([np.arange(groups) * per + p for p in range(per)])
    waves = np.repeat(waves[:, None, :], 2, axis=1).reshape(-1)
    part = np.broadcast_to(np.array([0, 1])[None, :, None], (per, 2, groups)).reshape(-1)
    cols = nlon // blocks
    edge = np.array([-2, -1, cols, cols + 1])
    halo = (edge[:, None] + np.arange(blocks)[None, :] * cols).reshape(-1) % nlon
    points = np.concatenate([np.arange(nlon), halo])
    angle = (waves[:, None] * points[None, :] % nlon) * (2.0 * math.pi / nlon)
    wave = np.where(part[:, None] == 0, np.cos(angle), -np.sin(angle)) / math.sqrt(nlon)
    factor = np.where(waves == 0, 1.0, 2.0)
    forward = wave[:, :nlon].astype(ml_dtypes.bfloat16)
    inverse = (wave * factor[:, None]).T.astype(ml_dtypes.bfloat16)
    return forward, np.ascontiguousarray(inverse)


class Sizes:
    def __init__(self, mesh, lat_rows, lon_cols, channels, wave_block, degrees):
        self.ni = mesh.shape["lat"]
        self.nj = mesh.shape["lon"]
        self.nq = channels // LANES
        self.nh = self.nj // self.nq
        self.groups = self.ni * self.nh
        self.rows = lat_rows
        self.trow = lat_rows // self.nh
        self.cols = lon_cols
        self.nlon = lon_cols * self.nj
        self.chan = channels
        self.wper = wave_block // self.nh
        self.deg = degrees
        self.nlat = lat_rows * self.ni
        self.step = 2
        self.chunks = self.trow // self.step
        self.mr = 2 * self.wper
        self.blk = self.step * self.mr
        self.deep = max(self.groups // 8, 1)
        self.late = self.mr // 3
        self.early = self.mr - self.late

    def turn(self, c, half):
        return c + half * (self.chunks - 1 - 2 * c)


def block_kernel(
    z,
    quad_hbm,
    neighbour_hbm,
    basis_hbm,
    disco_hbm,
    field_ref,
    leg_ref,
    fr_ref,
    fi_ref,
    fwd_ref,
    inv_ref,
    weight_ref,
    gain_ref,
    win_ref,
    bin_ref,
    wout_ref,
    bout_ref,
    block_out,
    spatial_out,
    quad_ref,
    neighbour,
    basis,
    disco,
    fbuf,
    cols_in,
    ltab,
    ltrans,
    fwd,
    inv,
    gr,
    gi,
    weight,
    gain,
    w_in,
    b_in,
    w_out,
    b_out,
    wrow,
    stage,
    stage_late,
    wide,
    wide_late,
    send1,
    recv1,
    send1_late,
    recv1_late,
    send2,
    recv2,
    wbuf,
    ebuf32,
    ebuf,
    vbuf,
    hbuf,
    padded,
    load_sem,
    a_send,
    a_recv,
    b_send,
    b_recv,
    c_send,
    c_recv,
    d_send,
    d_recv,
    e_send,
    e_recv,
    h_send,
    h_recv,
):
    i = lax.axis_index("lat")
    j = lax.axis_index("lon")
    h = j // z.nq
    q = j % z.nq
    me = i * z.nh + h
    lane0 = pl.multiple_of(q * LANES, LANES)
    G = z.groups
    early, late, step = z.early, z.late, z.step
    here = pl.ds(pl.multiple_of(j * z.cols, 16), z.cols)

    def load(n, src, dst):
        copy = pltpu.make_async_copy(src, dst, load_sem.at[n])
        copy.start()
        return copy

    field_load = load(0, field_ref, fbuf)
    leg_load = load(1, leg_ref.at[pl.ds(h * z.wper, z.wper)], ltab)
    fwd_load = load(2, fwd_ref, fwd)

    low = G // z.deep // 2
    deep = lax.rem(lax.div(me, low), z.deep)
    flat = lax.div(me, G // 2) * low + lax.rem(me, low)
    levels = [lax.rem(deep + 3 * a % z.deep, z.deep) for a in range(z.deep)]

    def each_peer(act):
        def shift(b, skip):
            other = lax.rem(flat + b, 2 * low)
            half = lax.div(other, low)
            side = lax.rem(other, low)
            column = lax.rem(side, z.nh) * z.nq + q
            first = half * (G // 2) + side
            row = half * (z.ni // 2) + lax.div(side, z.nh)
            for a in range(skip, z.deep):
                act(
                    first + levels[a] * low,
                    {"lat": row + levels[a] * (low // z.nh), "lon": column},
                )

        def body(b, carry):
            shift(b, 0)
            return carry

        shift(0, 1)
        lax.fori_loop(1, 2 * low, body, 0)

    barrier = pltpu.get_barrier_semaphore()

    def greet_lon(o, carry):
        hh = (h + o // (z.nq - 1)) % z.nh
        qq = (q + 1 + o % (z.nq - 1)) % z.nq
        pl.semaphore_signal(
            barrier, inc=1, device_id={"lat": i, "lon": hh * z.nq + qq}, device_id_type=MESH
        )
        return carry

    lon_only = z.nh * (z.nq - 1)
    with jax.named_scope("greet"):
        lax.fori_loop(0, lon_only, greet_lon, 0)
        each_peer(
            lambda peer, to: pl.semaphore_signal(
                barrier, inc=1, device_id=to, device_id_type=MESH
            )
        )
    rest = [
        load(n + 3, src, dst)
        for n, (src, dst) in enumerate(
            (
                (inv_ref, inv),
                (fr_ref.at[:, pl.ds(lane0, LANES)], gr),
                (fi_ref.at[:, pl.ds(lane0, LANES)], gi),
                (weight_ref, weight),
                (gain_ref, gain),
                (win_ref, w_in),
                (bin_ref, b_in),
                (wout_ref, w_out),
                (bout_ref, b_out),
                (quad_hbm, quad_ref),
                (neighbour_hbm, neighbour),
                (basis_hbm, basis),
                (disco_hbm, disco),
            )
        )
    ]
    field_load.wait()
    cols_in[:, here, :] = fbuf[pl.ds(h * z.trow, z.trow), :, pl.ds(lane0, LANES)]
    with jax.named_scope("barrier"):
        pl.semaphore_wait(barrier, lon_only + G - 1)

    def start_a(c):
        def send_a(o, carry):
            p = lax.rem(j + o, z.nj)
            hp = lax.div(p, z.nq)
            qp = lax.rem(p, z.nq)
            pltpu.make_async_remote_copy(
                src_ref=fbuf.at[
                    pl.ds(hp * z.trow + c * step, step),
                    :,
                    pl.ds(pl.multiple_of(qp * LANES, LANES), LANES),
                ],
                dst_ref=cols_in.at[pl.ds(c * step, step), here, :],
                send_sem=a_send,
                recv_sem=a_recv.at[c],
                device_id={"lat": i, "lon": p},
                device_id_type=MESH,
            ).start()
            return carry

        lax.fori_loop(1, z.nj, send_a, 0)

    def await_bytes(ref, sem):
        pltpu.make_async_copy(ref, ref, sem).wait()

    others = pl.ds(0, z.cols * (z.nj - 1))

    for c in range(z.chunks):
        start_a(c)
    leg_load.wait()
    with jax.named_scope("trans"):
        for w in range(z.wper):
            ltrans[w] = ltab[w].T
    rest[3].wait()
    rest[9].wait()
    for r in range(weight.shape[0]):
        wrow[r] = weight[r : r + 1, :]
    fwd_load.wait()

    def each_group(act):
        def body(s, carry):
            act(s)
            return carry

        lax.fori_loop(0, G, body, 0, unroll=8)

    def spread(src, dst, send_sem, recv_sem):
        def start(peer, to):
            pltpu.make_async_remote_copy(
                src_ref=src(peer),
                dst_ref=dst,
                send_sem=send_sem,
                recv_sem=recv_sem,
                device_id=to,
                device_id_type=MESH,
            ).start()

        with jax.named_scope("start"):
            each_peer(start)

    def rows_of(s, size):
        return pl.ds(pl.multiple_of(s * size, 8), size)

    for c in range(z.chunks):
        with jax.named_scope("a_wait"):
            await_bytes(cols_in.at[pl.ds(c * step, step), others, :], a_recv.at[c])
        with jax.named_scope("dft"):
            rhs = jnp.concatenate([cols_in[c * step + k] for k in range(step)], axis=1)
            spec = jnp.dot(fwd[...], rhs, preferred_element_type=F32)
            for k in range(step):
                quad = quad_ref[h * z.trow + c * step + k]
                part = spec[:, k * LANES : (k + 1) * LANES] * quad
                for p in range(z.mr):
                    piece = part[p * G : (p + 1) * G]
                    if p < early:
                        stage[pl.ds(k * early + p, G, stride=step * early), :] = piece
                    else:
                        at = (c * step + k) * late + p - early
                        stage_late[pl.ds(at, G, stride=z.trow * late), :] = piece

        def pack(s):
            send1[c, s] = stage[rows_of(s, step * early), :].astype(BF16)

        each_group(pack)
        recv1[c, me] = send1[c, me]
        spread(lambda peer: send1.at[c, peer], recv1.at[c, me], b_send.at[0], b_recv.at[c])

    def pack(s):
        send1_late[s] = stage_late[rows_of(s, z.trow * late), :].astype(BF16)

    each_group(pack)
    recv1_late[me] = send1_late[me]
    spread(
        lambda peer: send1_late.at[peer],
        recv1_late.at[me],
        b_send.at[1],
        b_recv.at[z.chunks],
    )

    for copy in rest[1:3]:
        copy.wait()

    def legendre(buf, count, first):
        for w in range(count // 2):
            weighted = jnp.concatenate(
                [buf[pl.ds(2 * w + r, z.nlat, stride=count), :] for r in range(2)], axis=1
            ).astype(BF16)
            coef = jnp.dot(ltab[first + w], weighted, preferred_element_type=F32)
            re = coef[:, :LANES]
            im = coef[:, LANES:]
            a = gr[...]
            b = gi[...]
            filt = jnp.concatenate([a * re - b * im, a * im + b * re], axis=1).astype(BF16)
            syn = jnp.dot(ltrans[first + w], filt, preferred_element_type=F32)
            for r in range(2):
                buf[pl.ds(2 * w + r, z.nlat, stride=count), :] = syn[
                    :, r * LANES : (r + 1) * LANES
                ]

    def pack_back(buf, count, c, at):
        def pack(s):
            first = (s * z.chunks + z.turn(c, lax.rem(s, z.nh))) * (step * count)
            rows = pl.ds(pl.multiple_of(first, 8), step * count)
            send2[c, s, at : at + step * count, :] = buf[rows, :].astype(BF16)

        each_group(pack)

    def spread_back(c):
        spread(lambda peer: send2.at[c, peer], recv2.at[c, me], c_send, c_recv.at[c])

    top = pl.ds(0, step * early)
    bottom = pl.ds(step * early, step * late)

    for c in range(z.chunks):
        with jax.named_scope("b_wait"):
            await_bytes(recv1.at[c, pl.ds(0, G - 1)], b_recv.at[c])

        def unpack(s):
            first = s * (z.trow * early) + c * step * early
            wide[pl.ds(pl.multiple_of(first, 8), step * early), :] = recv1[c, s].astype(F32)

        each_group(unpack)
    with jax.named_scope("legendre"):
        legendre(wide, early, 0)
    pack_back(wide, early, 0, 0)
    spread(
        lambda peer: send2.at[0, peer, top], recv2.at[0, me, top], c_send, c_recv.at[0]
    )
    for c in range(1, z.chunks):
        pack_back(wide, early, c, 0)
    with jax.named_scope("b_wait"):
        await_bytes(recv1_late.at[pl.ds(0, G - 1)], b_recv.at[z.chunks])

    def unpack(s):
        wide_late[rows_of(s, z.trow * late), :] = recv1_late[s].astype(F32)

    each_group(unpack)
    with jax.named_scope("legendre"):
        legendre(wide_late, late, early // 2)
    for c in range(z.chunks):
        pack_back(wide_late, late, c, step * early)
        if c == 0:
            spread(
                lambda peer: send2.at[0, peer, bottom],
                recv2.at[0, me, bottom],
                c_send,
                c_recv.at[0],
            )
        elif c == 1:
            spread_back(c)
        recv2[c, me] = send2[c, me]

    edge_rows = 4 * step
    span = z.rows + 2 * HALO
    moves = []
    for copy in rest[:1] + rest[4:9] + rest[10:]:
        copy.wait()

    def await_rows(c):
        await_bytes(wbuf.at[pl.ds(c * step, step), others, :], d_recv.at[c])
        await_bytes(ebuf.at[c, pl.ds(0, z.nj - 1)], e_recv.at[c])

    for c in range(z.chunks):
        with jax.named_scope("c_wait"):
            await_bytes(recv2.at[c, pl.ds(0, G - 1)], c_recv.at[c])

        def unpack(s):
            stage[rows_of(s, z.blk), :] = recv2[c, s].astype(F32)

        each_group(unpack)
        with jax.named_scope("idft"):
            modes = []
            for k in range(step):
                starts = [k * early + p for p in range(early)]
                starts += [step * early + k * late + p for p in range(late)]
                modes.append(
                    jnp.concatenate(
                        [stage[pl.ds(at, G, stride=z.blk), :] for at in starts], axis=0
                    )
                )
            full = jnp.dot(
                inv[...],
                jnp.concatenate(modes, axis=1).astype(BF16),
                preferred_element_type=F32,
            )
            for k in range(step):
                half = full[:, k * LANES : (k + 1) * LANES]
                wbuf[c * step + k] = half[: z.nlon].astype(BF16)
                for e in range(4):
                    at = z.nlon + e * z.nj
                    ebuf32[pl.ds(k * 4 + e, z.nj, stride=edge_rows), :] = half[at : at + z.nj]
            for p in range(z.nj):
                piece = ebuf32[p * edge_rows : (p + 1) * edge_rows, :]
                ebuf[c, p] = piece.astype(BF16).astype(F32)

        row = HALO + h * z.trow + z.turn(c, h) * step
        edge_at = pl.ds(pl.multiple_of(row * 4, 8), edge_rows)
        lanes = pl.ds(lane0, LANES)

        def send_d(o, carry):
            p = lax.rem(j + o, z.nj)
            there = pl.ds(pl.multiple_of(p * z.cols, 16), z.cols)
            for src, dst, ss, rs in (
                (
                    wbuf.at[pl.ds(c * step, step), there, :],
                    vbuf.at[pl.ds(row, step), :, lanes],
                    d_send,
                    d_recv.at[c],
                ),
                (ebuf.at[c, p], hbuf.at[edge_at, lanes], e_send, e_recv.at[c]),
            ):
                pltpu.make_async_remote_copy(
                    src_ref=src,
                    dst_ref=dst,
                    send_sem=ss,
                    recv_sem=rs,
                    device_id={"lat": i, "lon": p},
                    device_id_type=MESH,
                ).start()
            return carry

        lax.fori_loop(1, z.nj, send_d, 0)
        if c + 2 < z.chunks:
            spread_back(c + 2)
        vbuf[pl.ds(row, step), :, lanes] = wbuf[pl.ds(c * step, step), here, :]
        hbuf[edge_at, lanes] = ebuf[c, j]

        if c != 1:
            continue
        with jax.named_scope("h_start"):
            await_rows(0)
        last = z.rows + HALO
        for n, (src_row, dst_row, to) in enumerate(
            ((HALO, last, (i + z.ni - 1) % z.ni), (last - HALO, 0, (i + 1) % z.ni))
        ):
            for f, (src, dst) in enumerate(
                (
                    (vbuf.at[pl.ds(src_row, HALO)], vbuf.at[pl.ds(dst_row, HALO)]),
                    (
                        hbuf.at[pl.ds(src_row * 4, HALO * 4)],
                        hbuf.at[pl.ds(dst_row * 4, HALO * 4)],
                    ),
                )
            ):
                move = pltpu.make_async_remote_copy(
                    src_ref=src,
                    dst_ref=dst,
                    send_sem=h_send.at[n, f],
                    recv_sem=h_recv.at[n, f],
                    device_id={"lat": to, "lon": j},
                    device_id_type=MESH,
                )
                move.start()
                moves.append(move)

    def widen(first, count):
        def body(n, carry):
            pair = first + n
            for b in range(z.nq):
                lanes = slice(b * LANES, (b + 1) * LANES)
                edges = hbuf[pl.ds(pl.multiple_of(pair * 8, 8), 8), lanes]
                for k in range(2):
                    t = pair * 2 + k
                    padded[t, b, 8 : 8 + z.cols, :] = vbuf[t, :, lanes].astype(F32)
                    padded[t, b, 6:8, :] = edges[4 * k : 4 * k + 2]
                    padded[t, b, 8 + z.cols : 10 + z.cols, :] = edges[4 * k + 2 : 4 * k + 4]
            return carry

        with jax.named_scope("widen"):
            lax.fori_loop(0, count, body, 0)

    slots = neighbour.shape[1]

    def tile(pairs):
        for m, first in enumerate(pairs):

            def conv_row(k, carry):
                t = first + k
                for b in range(z.nq):
                    lanes = slice(b * LANES, (b + 1) * LANES)
                    total = padded[t + HALO, b, 8 : 8 + z.cols, :]
                    for s in range(slots):
                        at = neighbour[t, s]
                        coef = wrow[basis[t, s], :, lanes] * disco[t, s]
                        total = total + coef * padded[
                            t + at // 5, b, pl.ds(6 + at % 5, z.cols), :
                        ]
                    spatial_out[t, :, lanes] = total.astype(BF16)
                return carry

            with jax.named_scope("conv"):
                lax.fori_loop(0, 2, conv_row, 0)
        with jax.named_scope("mlp"):
            size = 4 * z.cols
            tokens = jnp.concatenate([spatial_out[pl.ds(first, 2)] for first in pairs], axis=0)
            tokens = tokens.reshape(size, z.chan).astype(F32)
            center = jnp.mean(tokens, axis=1, keepdims=True)
            tokens = tokens - center
            spread_ = jnp.mean(tokens * tokens, axis=1, keepdims=True)
            normed = (tokens * lax.rsqrt(spread_ + 1e-05) * gain[...]).astype(BF16)
            hidden = jnp.dot(normed, w_in[...], preferred_element_type=F32) + b_in[...]
            hidden = jax.nn.gelu(hidden).astype(BF16)
            total = jnp.dot(hidden, w_out[...], preferred_element_type=F32) + b_out[...]
            total = total.reshape(4, z.cols, z.chan)
            for m, first in enumerate(pairs):
                skip = fbuf[pl.ds(first, 2)].astype(F32)
                block_out[pl.ds(first, 2)] = (total[2 * m : 2 * m + 2] + skip).astype(BF16)

    with jax.named_scope("h_wait"):
        await_rows(1)
        for move in moves:
            move.wait()
    near = span // 4 - 1
    widen(0, near)
    widen(span // 2 - near, near)

    @pl.when(i == 0)
    def _():
        padded[:HALO] = jnp.zeros((HALO,) + padded.shape[1:], F32)

    @pl.when(i == z.ni - 1)
    def _():
        padded[span - HALO :] = jnp.zeros((HALO,) + padded.shape[1:], F32)

    tile((0, z.rows - 2))
    with jax.named_scope("d_wait"):
        for c in range(2, z.chunks):
            await_rows(c)
    widen(near, span // 2 - 2 * near)

    def rest_tile(n, carry):
        tile((4 * n - 2, 4 * n))
        return carry

    lax.fori_loop(1, z.rows // 4, rest_tile, 0)

    with jax.named_scope("drain"):
        await_bytes(wbuf.at[:, others, :], a_send)
        await_bytes(send1.at[:, pl.ds(0, G - 1)], b_send.at[0])
        await_bytes(send1_late.at[pl.ds(0, G - 1)], b_send.at[1])
        await_bytes(send2.at[:, pl.ds(0, G - 1)], c_send)
        await_bytes(wbuf.at[:, others, :], d_send)
        await_bytes(ebuf.at[:, pl.ds(0, z.nj - 1)], e_send)


def block(z, quad, neighbour, basis, disco, *arrays):
    field, legendre, fr, fi, fwd, inv, weight, gain, w_in, b_in, w_out, b_out = arrays
    hbm = pl.BlockSpec(memory_space=pl.ANY)
    dma = pltpu.SemaphoreType.DMA
    span = z.rows + 2 * HALO

    def vmem(dtype, *dims):
        return pltpu.VMEM(dims, dtype)

    wide = z.groups * z.trow
    return pl.pallas_call(
        functools.partial(block_kernel, z),
        name="block",
        out_shape=(pltpu.VMEM(field.shape, BF16),) * 2,
        in_specs=[hbm] * 4 + [hbm] * len(arrays),
        out_specs=(pl.BlockSpec(memory_space=pltpu.VMEM),) * 2,
        scratch_shapes=[pltpu.SMEM(x.shape, x.dtype) for x in (quad, neighbour, basis, disco)]
        + [
            vmem(BF16, *field.shape),
            vmem(BF16, z.trow, z.nlon, LANES),
            vmem(BF16, z.wper, z.deg, z.nlat),
            vmem(BF16, z.wper, z.nlat, z.deg),
            vmem(BF16, *fwd.shape),
            vmem(BF16, *inv.shape),
            vmem(F32, z.deg, LANES),
            vmem(F32, z.deg, LANES),
            vmem(F32, *weight.shape),
            vmem(F32, *gain.shape),
            vmem(BF16, *w_in.shape),
            vmem(F32, *b_in.shape),
            vmem(BF16, *w_out.shape),
            vmem(F32, *b_out.shape),
            vmem(F32, weight.shape[0], 1, z.chan),
            vmem(F32, z.groups * z.blk, LANES),
            vmem(F32, wide * z.late, LANES),
            vmem(F32, wide * z.early, LANES),
            vmem(F32, wide * z.late, LANES),
            vmem(BF16, z.chunks, z.groups, z.step * z.early, LANES),
            vmem(BF16, z.chunks, z.groups, z.step * z.early, LANES),
            vmem(BF16, z.groups, z.trow * z.late, LANES),
            vmem(BF16, z.groups, z.trow * z.late, LANES),
            vmem(BF16, z.chunks, z.groups, z.blk, LANES),
            vmem(BF16, z.chunks, z.groups, z.blk, LANES),
            vmem(BF16, z.trow, z.nlon, LANES),
            vmem(F32, z.nj * 4 * z.step, LANES),
            vmem(F32, z.chunks, z.nj, 4 * z.step, LANES),
            vmem(BF16, span, z.cols, z.chan),
            vmem(F32, span * 4, z.chan),
            vmem(F32, span, z.nq, z.cols + 16, LANES),
            dma((16,)),
            dma,
            dma((z.chunks,)),
            dma((2,)),
            dma((z.chunks + 1,)),
            dma,
            dma((z.chunks,)),
            dma,
            dma((z.chunks,)),
            dma,
            dma((z.chunks,)),
            dma((2, 2)),
            dma((2, 2)),
        ],
        compiler_params=pltpu.CompilerParams(
            collective_id=0, has_side_effects=True, vmem_limit_bytes=56 << 20
        ),
    )(quad, neighbour, basis, disco, *arrays)


def shards(
    mesh,
    field,
    quad_weight,
    legendre,
    filter_real,
    filter_imag,
    neighbour,
    basis,
    disco_quad,
    disco_weight,
    norm_gain,
    w_in,
    b_in,
    w_out,
    b_out,
):
    lat_rows, lon_cols, channels = field.shape
    z = Sizes(mesh, lat_rows, lon_cols, channels, legendre.shape[0], legendre.shape[1])
    fwd, inv = tables(z.nlon, z.wper * z.groups, z.groups, z.nj)
    return block(
        z,
        quad_weight,
        neighbour,
        basis,
        disco_quad,
        field,
        legendre,
        filter_real,
        filter_imag,
        jnp.asarray(fwd),
        jnp.asarray(inv),
        disco_weight,
        norm_gain[None],
        w_in,
        b_in[None],
        w_out,
        b_out[None],
    )


def solution(mesh):
    placed = (
        P("lat", "lon", None),
        P("lat"),
        P("lat", None, None),
        P(),
        P(),
        P("lat", None),
        P("lat", None),
        P("lat", None),
        P(),
        P(),
        P(),
        P(),
        P(),
        P(),
    )
    return jax.shard_map(
        functools.partial(shards, mesh),
        mesh=mesh,
        in_specs=placed,
        out_specs=(P("lat", "lon", None), P("lat", "lon", None)),
        check_vma=False,
    )
```

```python
import functools
import math

import jax
import jax.numpy as jnp
import ml_dtypes
import numpy as np
from jax import lax
from jax.experimental import pallas as pl
from jax.experimental.pallas import tpu as pltpu
from jax.sharding import PartitionSpec as P

HALO = 2
LANES = 128
MESH = pl.DeviceIdType.MESH
BF16 = jnp.bfloat16
F32 = jnp.float32


def fourier_table(nlon, mmax, groups, blocks):
    per = mmax // groups
    waves = np.stack([np.arange(groups) * per + p for p in range(per)])
    waves = np.repeat(waves[:, None, :], 2, axis=1).reshape(-1)
    part = np.broadcast_to(np.array([0, 1])[None, :, None], (per, 2, groups)).reshape(-1)
    cols = nlon // blocks
    edge = np.array([-2, -1, cols, cols + 1])
    halo = (edge[:, None] + np.arange(blocks)[None, :] * cols).reshape(-1) % nlon
    points = np.concatenate([np.arange(nlon), halo])
    angle = (points[:, None] * waves[None, :] % nlon) * (2.0 * math.pi / nlon)
    wave = np.where(part[None, :] == 0, np.cos(angle), -np.sin(angle)) / math.sqrt(nlon)
    return wave.astype(ml_dtypes.bfloat16)


class Sizes:
    def __init__(self, mesh, lat_rows, lon_cols, channels, wave_block, degrees):
        self.ni = mesh.shape["lat"]
        self.nj = mesh.shape["lon"]
        self.nq = channels // LANES
        self.nh = self.nj // self.nq
        self.groups = self.ni * self.nh
        self.rows = lat_rows
        self.trow = lat_rows // self.nh
        self.cols = lon_cols
        self.nlon = lon_cols * self.nj
        self.chan = channels
        self.wper = wave_block // self.nh
        self.deg = degrees
        self.nlat = lat_rows * self.ni
        self.step = 2
        self.chunks = self.trow // self.step
        self.mr = 2 * self.wper
        self.blk = self.step * self.mr
        self.deep = max(self.groups // 8, 1)
        self.late = self.mr // 3
        self.early = self.mr - self.late

    def turn(self, c, half):
        return c + half * (self.chunks - 1 - 2 * c)


def block_kernel(
    z,
    quad_hbm,
    neighbour_hbm,
    basis_hbm,
    disco_hbm,
    field_ref,
    leg_ref,
    fr_ref,
    fi_ref,
    inv_ref,
    weight_ref,
    gain_ref,
    win_ref,
    bin_ref,
    wout_ref,
    bout_ref,
    block_out,
    spatial_out,
    quad_ref,
    neighbour,
    basis,
    disco,
    fbuf,
    fblocks,
    cols_in,
    ltab,
    ltrans,
    fwd,
    inv,
    gr,
    gi,
    weight,
    gain,
    w_in,
    b_in,
    w_out,
    b_out,
    wrow,
    stage,
    stage_late,
    wide,
    wide_late,
    send1,
    recv1,
    send1_late,
    recv1_late,
    send2,
    recv2,
    wbuf,
    ebuf32,
    ebuf,
    vbuf,
    hbuf,
    padded,
    load_sem,
    a_send,
    a_recv,
    b_send,
    b_recv,
    c_send,
    c_recv,
    d_send,
    d_recv,
    e_send,
    e_recv,
    h_send,
    h_recv,
):
    i = lax.axis_index("lat")
    j = lax.axis_index("lon")
    h = j // z.nq
    q = j % z.nq
    me = i * z.nh + h
    lane0 = pl.multiple_of(q * LANES, LANES)
    G = z.groups
    early, late, step = z.early, z.late, z.step
    here = pl.ds(pl.multiple_of(j * z.cols, 16), z.cols)

    def load(n, src, dst):
        copy = pltpu.make_async_copy(src, dst, load_sem.at[n])
        copy.start()
        return copy

    field_load = load(0, field_ref, fbuf)
    leg_load = load(1, leg_ref.at[pl.ds(h * z.wper, z.wper)], ltab)
    table_load = load(2, inv_ref, inv)

    low = G // z.deep // 2
    deep = lax.rem(lax.div(me, low), z.deep)
    flat = lax.div(me, G // 2) * low + lax.rem(me, low)
    levels = [lax.rem(deep + 3 * a % z.deep, z.deep) for a in range(z.deep)]

    def each_peer(act):
        def shift(b, skip):
            other = lax.rem(flat + b, 2 * low)
            half = lax.div(other, low)
            side = lax.rem(other, low)
            column = lax.rem(side, z.nh) * z.nq + q
            first = half * (G // 2) + side
            row = half * (z.ni // 2) + lax.div(side, z.nh)
            for a in range(skip, z.deep):
                act(
                    first + levels[a] * low,
                    {"lat": row + levels[a] * (low // z.nh), "lon": column},
                )

        def body(b, carry):
            shift(b, 0)
            return carry

        shift(0, 1)
        lax.fori_loop(1, 2 * low, body, 0)

    barrier = pltpu.get_barrier_semaphore()

    def greet_lon(o, carry):
        hh = (h + o // (z.nq - 1)) % z.nh
        qq = (q + 1 + o % (z.nq - 1)) % z.nq
        pl.semaphore_signal(
            barrier, inc=1, device_id={"lat": i, "lon": hh * z.nq + qq}, device_id_type=MESH
        )
        return carry

    lon_only = z.nh * (z.nq - 1)
    with jax.named_scope("greet"):
        lax.fori_loop(0, lon_only, greet_lon, 0)
        each_peer(
            lambda peer, to: pl.semaphore_signal(
                barrier, inc=1, device_id=to, device_id_type=MESH
            )
        )
    rest = [
        load(n + 3, src, dst)
        for n, (src, dst) in enumerate(
            (
                (fr_ref.at[:, pl.ds(lane0, LANES)], gr),
                (fi_ref.at[:, pl.ds(lane0, LANES)], gi),
                (weight_ref, weight),
                (gain_ref, gain),
                (win_ref, w_in),
                (bin_ref, b_in),
                (wout_ref, w_out),
                (bout_ref, b_out),
                (quad_hbm, quad_ref),
                (neighbour_hbm, neighbour),
                (basis_hbm, basis),
                (disco_hbm, disco),
            )
        )
    ]
    field_load.wait()
    for b in range(z.nq):
        fblocks[b] = fbuf[:, :, b * LANES : (b + 1) * LANES]
    cols_in[:, here, :] = fblocks[q, pl.ds(h * z.trow, z.trow)]
    table_load.wait()
    with jax.named_scope("trans"):
        fwd[...] = inv[: z.nlon, :].T
    with jax.named_scope("barrier"):
        pl.semaphore_wait(barrier, lon_only + G - 1)

    def start_a(c):
        def send_a(o, carry):
            p = lax.rem(j + o, z.nj)
            hp = lax.div(p, z.nq)
            qp = lax.rem(p, z.nq)
            pltpu.make_async_remote_copy(
                src_ref=fblocks.at[qp, pl.ds(hp * z.trow + c * step, step)],
                dst_ref=cols_in.at[pl.ds(c * step, step), here, :],
                send_sem=a_send,
                recv_sem=a_recv.at[c],
                device_id={"lat": i, "lon": p},
                device_id_type=MESH,
            ).start()
            return carry

        lax.fori_loop(1, z.nj, send_a, 0)

    def await_bytes(ref, sem):
        pltpu.make_async_copy(ref, ref, sem).wait()

    others = pl.ds(0, z.cols * (z.nj - 1))

    for c in range(z.chunks):
        start_a(c)
    leg_load.wait()
    with jax.named_scope("trans"):
        for w in range(z.wper):
            ltrans[w] = ltab[w].T
    rest[2].wait()
    rest[8].wait()
    for r in range(weight.shape[0]):
        wrow[r] = weight[r : r + 1, :]

    def each_group(act):
        def body(s, carry):
            act(s)
            return carry

        lax.fori_loop(0, G, body, 0, unroll=8)

    def spread(src, dst, send_sem, recv_sem):
        def start(peer, to):
            pltpu.make_async_remote_copy(
                src_ref=src(peer),
                dst_ref=dst,
                send_sem=send_sem,
                recv_sem=recv_sem,
                device_id=to,
                device_id_type=MESH,
            ).start()

        with jax.named_scope("start"):
            each_peer(start)

    def rows_of(s, size):
        return pl.ds(pl.multiple_of(s * size, 8), size)

    for c in range(z.chunks):
        with jax.named_scope("a_wait"):
            await_bytes(cols_in.at[pl.ds(c * step, step), others, :], a_recv.at[c])
        with jax.named_scope("dft"):
            rhs = jnp.concatenate([cols_in[c * step + k] for k in range(step)], axis=1)
            spec = jnp.dot(fwd[...], rhs, preferred_element_type=F32)
            for k in range(step):
                quad = quad_ref[h * z.trow + c * step + k]
                part = spec[:, k * LANES : (k + 1) * LANES] * quad
                for p in range(z.mr):
                    piece = part[p * G : (p + 1) * G]
                    if p < early:
                        stage[pl.ds(k * early + p, G, stride=step * early), :] = piece
                    else:
                        at = (c * step + k) * late + p - early
                        stage_late[pl.ds(at, G, stride=z.trow * late), :] = piece

        def pack(s):
            send1[c, s] = stage[rows_of(s, step * early), :].astype(BF16)

        each_group(pack)
        recv1[c, me] = send1[c, me]
        spread(lambda peer: send1.at[c, peer], recv1.at[c, me], b_send.at[0], b_recv.at[c])

    def pack(s):
        send1_late[s] = stage_late[rows_of(s, z.trow * late), :].astype(BF16)

    each_group(pack)
    recv1_late[me] = send1_late[me]
    spread(
        lambda peer: send1_late.at[peer],
        recv1_late.at[me],
        b_send.at[1],
        b_recv.at[z.chunks],
    )

    for copy in rest[:2]:
        copy.wait()

    def legendre(buf, count, first):
        for w in range(count // 2):
            weighted = jnp.concatenate(
                [buf[pl.ds(2 * w + r, z.nlat, stride=count), :] for r in range(2)], axis=1
            ).astype(BF16)
            coef = jnp.dot(ltab[first + w], weighted, preferred_element_type=F32)
            re = coef[:, :LANES]
            im = coef[:, LANES:]
            a = gr[...]
            b = gi[...]
            filt = jnp.concatenate([a * re - b * im, a * im + b * re], axis=1).astype(BF16)
            syn = jnp.dot(ltrans[first + w], filt, preferred_element_type=F32)
            twice = jnp.where(me + first + w == 0, 1.0, 2.0) if first + w == 0 else 2.0
            for r in range(2):
                buf[pl.ds(2 * w + r, z.nlat, stride=count), :] = (
                    syn[:, r * LANES : (r + 1) * LANES] * twice
                )

    def pack_back(buf, count, c, at):
        def pack(s):
            first = (s * z.chunks + z.turn(c, lax.rem(s, z.nh))) * (step * count)
            rows = pl.ds(pl.multiple_of(first, 8), step * count)
            send2[c, s, at : at + step * count, :] = buf[rows, :].astype(BF16)

        each_group(pack)

    def spread_back(c):
        spread(lambda peer: send2.at[c, peer], recv2.at[c, me], c_send, c_recv.at[c])

    top = pl.ds(0, step * early)
    bottom = pl.ds(step * early, step * late)

    for c in range(z.chunks):
        with jax.named_scope("b_wait"):
            await_bytes(recv1.at[c, pl.ds(0, G - 1)], b_recv.at[c])

        def unpack(s):
            first = s * (z.trow * early) + c * step * early
            wide[pl.ds(pl.multiple_of(first, 8), step * early), :] = recv1[c, s].astype(F32)

        each_group(unpack)
    with jax.named_scope("legendre"):
        legendre(wide, early, 0)
    pack_back(wide, early, 0, 0)
    spread(
        lambda peer: send2.at[0, peer, top], recv2.at[0, me, top], c_send, c_recv.at[0]
    )
    for c in range(1, z.chunks):
        pack_back(wide, early, c, 0)
    with jax.named_scope("b_wait"):
        await_bytes(recv1_late.at[pl.ds(0, G - 1)], b_recv.at[z.chunks])

    def unpack(s):
        wide_late[rows_of(s, z.trow * late), :] = recv1_late[s].astype(F32)

    each_group(unpack)
    with jax.named_scope("legendre"):
        legendre(wide_late, late, early // 2)
    for c in range(z.chunks):
        pack_back(wide_late, late, c, step * early)
        if c == 0:
            spread(
                lambda peer: send2.at[0, peer, bottom],
                recv2.at[0, me, bottom],
                c_send,
                c_recv.at[0],
            )
        elif c == 1:
            spread_back(c)
        recv2[c, me] = send2[c, me]

    edge_rows = 4 * step
    span = z.rows + 2 * HALO
    moves = []
    for copy in rest[3:8] + rest[9:]:
        copy.wait()

    def await_rows(c):
        await_bytes(wbuf.at[pl.ds(c * step, step), others, :], d_recv.at[c])
        await_bytes(ebuf.at[c, pl.ds(0, z.nj - 1)], e_recv.at[c])

    for c in range(z.chunks):
        with jax.named_scope("c_wait"):
            await_bytes(recv2.at[c, pl.ds(0, G - 1)], c_recv.at[c])

        def unpack(s):
            stage[rows_of(s, z.blk), :] = recv2[c, s].astype(F32)

        each_group(unpack)
        with jax.named_scope("idft"):
            modes = []
            for k in range(step):
                starts = [k * early + p for p in range(early)]
                starts += [step * early + k * late + p for p in range(late)]
                modes.append(
                    jnp.concatenate(
                        [stage[pl.ds(at, G, stride=z.blk), :] for at in starts], axis=0
                    )
                )
            full = jnp.dot(
                inv[...],
                jnp.concatenate(modes, axis=1).astype(BF16),
                preferred_element_type=F32,
            )
            for k in range(step):
                half = full[:, k * LANES : (k + 1) * LANES]
                wbuf[c * step + k] = half[: z.nlon].astype(BF16)
                for e in range(4):
                    at = z.nlon + e * z.nj
                    ebuf32[pl.ds(k * 4 + e, z.nj, stride=edge_rows), :] = half[at : at + z.nj]
            for p in range(z.nj):
                piece = ebuf32[p * edge_rows : (p + 1) * edge_rows, :]
                ebuf[c, p] = piece.astype(BF16).astype(F32)

        row = HALO + h * z.trow + z.turn(c, h) * step
        edge_at = pl.ds(pl.multiple_of(row * 4, 8), edge_rows)
        lanes = pl.ds(lane0, LANES)

        def send_d(o, carry):
            p = lax.rem(j + o, z.nj)
            there = pl.ds(pl.multiple_of(p * z.cols, 16), z.cols)
            for src, dst, ss, rs in (
                (
                    wbuf.at[pl.ds(c * step, step), there, :],
                    vbuf.at[q, pl.ds(row, step)],
                    d_send,
                    d_recv.at[c],
                ),
                (ebuf.at[c, p], hbuf.at[edge_at, lanes], e_send, e_recv.at[c]),
            ):
                pltpu.make_async_remote_copy(
                    src_ref=src,
                    dst_ref=dst,
                    send_sem=ss,
                    recv_sem=rs,
                    device_id={"lat": i, "lon": p},
                    device_id_type=MESH,
                ).start()
            return carry

        lax.fori_loop(1, z.nj, send_d, 0)
        if c + 2 < z.chunks:
            spread_back(c + 2)
        vbuf[q, pl.ds(row, step)] = wbuf[pl.ds(c * step, step), here, :]
        hbuf[edge_at, lanes] = ebuf[c, j]

        if c != 1:
            continue
        with jax.named_scope("h_start"):
            await_rows(0)
        last = z.rows + HALO
        for n, (src_row, dst_row, to) in enumerate(
            ((HALO, last, (i + z.ni - 1) % z.ni), (last - HALO, 0, (i + 1) % z.ni))
        ):
            for f, (src, dst) in enumerate(
                (
                    (vbuf.at[:, pl.ds(src_row, HALO)], vbuf.at[:, pl.ds(dst_row, HALO)]),
                    (
                        hbuf.at[pl.ds(src_row * 4, HALO * 4)],
                        hbuf.at[pl.ds(dst_row * 4, HALO * 4)],
                    ),
                )
            ):
                move = pltpu.make_async_remote_copy(
                    src_ref=src,
                    dst_ref=dst,
                    send_sem=h_send.at[n, f],
                    recv_sem=h_recv.at[n, f],
                    device_id={"lat": to, "lon": j},
                    device_id_type=MESH,
                )
                move.start()
                moves.append(move)

    def widen(first, count):
        def body(n, carry):
            pair = first + n
            for b in range(z.nq):
                lanes = slice(b * LANES, (b + 1) * LANES)
                edges = hbuf[pl.ds(pl.multiple_of(pair * 8, 8), 8), lanes]
                for k in range(2):
                    t = pair * 2 + k
                    padded[t, b, 8 : 8 + z.cols, :] = vbuf[b, t].astype(F32)
                    padded[t, b, 6:8, :] = edges[4 * k : 4 * k + 2]
                    padded[t, b, 8 + z.cols : 10 + z.cols, :] = edges[4 * k + 2 : 4 * k + 4]
            return carry

        with jax.named_scope("widen"):
            lax.fori_loop(0, count, body, 0)

    slots = neighbour.shape[1]

    def tile(pairs):
        def conv_row(t):
            taps = []
            for s in range(slots):
                at = neighbour[t, s]
                down = lax.div(at, 5)
                taps.append((t + down, 6 + at - 5 * down, basis[t, s], disco[t, s]))
            for b in range(z.nq):
                lanes = slice(b * LANES, (b + 1) * LANES)
                total = padded[t + HALO, b, 8 : 8 + z.cols, :]
                for row, col, kind, amount in taps:
                    coef = wrow[kind, :, lanes] * amount
                    total = total + coef * padded[row, b, pl.ds(col, z.cols), :]
                spatial_out[t, :, lanes] = total.astype(BF16)

        with jax.named_scope("conv"):
            for first in pairs:
                for k in range(2):
                    conv_row(first + k)
        with jax.named_scope("mlp"):
            size = 4 * z.cols
            tokens = jnp.concatenate([spatial_out[pl.ds(first, 2)] for first in pairs], axis=0)
            tokens = tokens.reshape(size, z.chan).astype(F32)
            center = jnp.mean(tokens, axis=1, keepdims=True)
            tokens = tokens - center
            spread_ = jnp.mean(tokens * tokens, axis=1, keepdims=True)
            normed = (tokens * lax.rsqrt(spread_ + 1e-05) * gain[...]).astype(BF16)
            hidden = jnp.dot(normed, w_in[...], preferred_element_type=F32) + b_in[...]
            hidden = jax.nn.gelu(hidden).astype(BF16)
            total = jnp.dot(hidden, w_out[...], preferred_element_type=F32) + b_out[...]
            total = total.reshape(4, z.cols, z.chan)
            for m, first in enumerate(pairs):
                skip = fbuf[pl.ds(first, 2)].astype(F32)
                block_out[pl.ds(first, 2)] = (total[2 * m : 2 * m + 2] + skip).astype(BF16)

    with jax.named_scope("h_wait"):
        await_rows(1)
        for move in moves:
            move.wait()
    near = span // 4 - 1
    widen(0, near)
    widen(span // 2 - near, near)

    @pl.when(i == 0)
    def _():
        padded[:HALO] = jnp.zeros((HALO,) + padded.shape[1:], F32)

    @pl.when(i == z.ni - 1)
    def _():
        padded[span - HALO :] = jnp.zeros((HALO,) + padded.shape[1:], F32)

    tile((0, z.rows - 2))
    with jax.named_scope("d_wait"):
        for c in range(2, z.chunks):
            await_rows(c)
    widen(near, span // 2 - 2 * near)

    def rest_tile(n, carry):
        tile((4 * n - 2, 4 * n))
        return carry

    lax.fori_loop(1, z.rows // 4, rest_tile, 0)

    with jax.named_scope("drain"):
        await_bytes(wbuf.at[:, others, :], a_send)
        await_bytes(send1.at[:, pl.ds(0, G - 1)], b_send.at[0])
        await_bytes(send1_late.at[pl.ds(0, G - 1)], b_send.at[1])
        await_bytes(send2.at[:, pl.ds(0, G - 1)], c_send)
        await_bytes(wbuf.at[:, others, :], d_send)
        await_bytes(ebuf.at[:, pl.ds(0, z.nj - 1)], e_send)


def block(z, quad, neighbour, basis, disco, *arrays):
    field, legendre, fr, fi, inv, weight, gain, w_in, b_in, w_out, b_out = arrays
    hbm = pl.BlockSpec(memory_space=pl.ANY)
    dma = pltpu.SemaphoreType.DMA
    span = z.rows + 2 * HALO

    def vmem(dtype, *dims):
        return pltpu.VMEM(dims, dtype)

    wide = z.groups * z.trow
    return pl.pallas_call(
        functools.partial(block_kernel, z),
        name="block",
        out_shape=(pltpu.VMEM(field.shape, BF16),) * 2,
        in_specs=[hbm] * 4 + [hbm] * len(arrays),
        out_specs=(pl.BlockSpec(memory_space=pltpu.VMEM),) * 2,
        scratch_shapes=[pltpu.SMEM(x.shape, x.dtype) for x in (quad, neighbour, basis, disco)]
        + [
            vmem(BF16, *field.shape),
            vmem(BF16, z.nq, z.rows, z.cols, LANES),
            vmem(BF16, z.trow, z.nlon, LANES),
            vmem(BF16, z.wper, z.deg, z.nlat),
            vmem(BF16, z.wper, z.nlat, z.deg),
            vmem(BF16, inv.shape[1], z.nlon),
            vmem(BF16, *inv.shape),
            vmem(F32, z.deg, LANES),
            vmem(F32, z.deg, LANES),
            vmem(F32, *weight.shape),
            vmem(F32, *gain.shape),
            vmem(BF16, *w_in.shape),
            vmem(F32, *b_in.shape),
            vmem(BF16, *w_out.shape),
            vmem(F32, *b_out.shape),
            vmem(F32, weight.shape[0], 1, z.chan),
            vmem(F32, z.groups * z.blk, LANES),
            vmem(F32, wide * z.late, LANES),
            vmem(F32, wide * z.early, LANES),
            vmem(F32, wide * z.late, LANES),
            vmem(BF16, z.chunks, z.groups, z.step * z.early, LANES),
            vmem(BF16, z.chunks, z.groups, z.step * z.early, LANES),
            vmem(BF16, z.groups, z.trow * z.late, LANES),
            vmem(BF16, z.groups, z.trow * z.late, LANES),
            vmem(BF16, z.chunks, z.groups, z.blk, LANES),
            vmem(BF16, z.chunks, z.groups, z.blk, LANES),
            vmem(BF16, z.trow, z.nlon, LANES),
            vmem(F32, z.nj * 4 * z.step, LANES),
            vmem(F32, z.chunks, z.nj, 4 * z.step, LANES),
            vmem(BF16, z.nq, span, z.cols, LANES),
            vmem(F32, span * 4, z.chan),
            vmem(F32, span, z.nq, z.cols + 16, LANES),
            dma((16,)),
            dma,
            dma((z.chunks,)),
            dma((2,)),
            dma((z.chunks + 1,)),
            dma,
            dma((z.chunks,)),
            dma,
            dma((z.chunks,)),
            dma,
            dma((z.chunks,)),
            dma((2, 2)),
            dma((2, 2)),
        ],
        compiler_params=pltpu.CompilerParams(
            collective_id=0, has_side_effects=True, vmem_limit_bytes=56 << 20
        ),
    )(quad, neighbour, basis, disco, *arrays)


def shards(
    mesh,
    field,
    quad_weight,
    legendre,
    filter_real,
    filter_imag,
    neighbour,
    basis,
    disco_quad,
    disco_weight,
    norm_gain,
    w_in,
    b_in,
    w_out,
    b_out,
):
    lat_rows, lon_cols, channels = field.shape
    z = Sizes(mesh, lat_rows, lon_cols, channels, legendre.shape[0], legendre.shape[1])
    table = fourier_table(z.nlon, z.wper * z.groups, z.groups, z.nj)
    return block(
        z,
        quad_weight,
        neighbour,
        basis,
        disco_quad,
        field,
        legendre,
        filter_real,
        filter_imag,
        jnp.asarray(table),
        disco_weight,
        norm_gain[None],
        w_in,
        b_in[None],
        w_out,
        b_out[None],
    )


def solution(mesh):
    placed = (
        P("lat", "lon", None),
        P("lat"),
        P("lat", None, None),
        P(),
        P(),
        P("lat", None),
        P("lat", None),
        P("lat", None),
        P(),
        P(),
        P(),
        P(),
        P(),
        P(),
    )
    return jax.shard_map(
        functools.partial(shards, mesh),
        mesh=mesh,
        in_specs=placed,
        out_specs=(P("lat", "lon", None), P("lat", "lon", None)),
        check_vma=False,
    )
```
